32 devices in a mesh: dp: 4 (over z), tp: 8 (over y, x, core).
Axes of the slice: x: 2, y: 2, z: 4, core: 2. Of those that a mesh axis runs over, the one named last changes fastest.
Arguments:
- hidden: bfloat16 [2048, 640], P(('dp', 'tp'))
- w_unembed: bfloat16 [640, 262144], P(('dp', 'tp'))
Outputs:
- output: bfloat16 [2048, 262144], P(None, ('dp', 'tp'))
All inputs are finite; a program needn't handle non-finite values.
Results may differ from the reference program's by a relative error of at most 0.001.
Values are sent between devices in bfloat16 or wider.
A program may use at most 1 GiB of HBM per device.

```python
import jax
import jax.numpy as jnp
from jax import lax

TOTAL_ROWS = 2048
MODEL_DIM = 640
VOCAB_SIZE = 262144
NUM_SHARDS = 32


def setup_inputs(seed: int = 0) -> dict:
    key_hidden, key_weight = jax.random.split(jax.random.key(seed))
    hidden = jax.random.normal(key_hidden, (TOTAL_ROWS, MODEL_DIM), jnp.float32)
    weight = jax.random.normal(key_weight, (MODEL_DIM, VOCAB_SIZE), jnp.float32) * MODEL_DIM ** -0.5
    return {"hidden": hidden.astype(jnp.bfloat16), "w_unembed": weight.astype(jnp.bfloat16)}


def reference(hidden, w_unembed):
    block_rows = TOTAL_ROWS // NUM_SHARDS

    def row_block(hid_blk):
        return jnp.dot(hid_blk, w_unembed, preferred_element_type=jnp.float32).astype(jnp.bfloat16)

    logits = lax.map(row_block, hidden.reshape(NUM_SHARDS, block_rows, MODEL_DIM))
    return logits.reshape(TOTAL_ROWS, VOCAB_SIZE)
```

```python
import functools, jax, jax.numpy as jnp
from jax import lax
from jax.experimental import pallas as pl
from jax.experimental.pallas import tpu as pltpu
from jax.sharding import PartitionSpec as P

def mm(h_ref, a1, a2, b, y_in, y_ref):
    nb = pl.program_id(0)
    del y_in
    acc = jnp.dot(h_ref[:, 0:256], a1[...], preferred_element_type=jnp.float32)
    acc += jnp.dot(h_ref[:, 256:512], a2[...], preferred_element_type=jnp.float32)
    half = (nb * 2) // pl.num_programs(0)
    off = pl.multiple_of(512 + half * 256, 256)
    acc += jnp.dot(h_ref[:, pl.ds(off, 256)], b[...], preferred_element_type=jnp.float32)
    y_ref[...] = acc.astype(jnp.bfloat16)

def chunk_mm(h4, r, y, c, nc, tn=512, M=2048):
    nt = nc // tn
    specs = [pl.BlockSpec((M, 1024), lambda j: (0, 0)),
             pl.BlockSpec((256, tn), lambda j: (0, j)),
             pl.BlockSpec((256, tn), lambda j: (0, nt + j)),
             pl.BlockSpec((256, tn), lambda j: (0, 2 * nt + j % (nt // 2)))]
    kw = {}
    args = (h4, r, r, r)
    if y is not None:
        specs.append(pl.BlockSpec(memory_space=pl.ANY)); args += (y,); kw = dict(input_output_aliases={4: 0})
        body = mm
    else:
        body = lambda h, a1, a2, b, o: mm(h, a1, a2, b, None, o)
    return pl.pallas_call(body, grid=(nt,), out_shape=jax.ShapeDtypeStruct((2048, 8192), jnp.bfloat16),
        in_specs=specs, out_specs=pl.BlockSpec((M, tn), lambda j: (0, c * nt + j)),
        cost_estimate=pl.CostEstimate(flops=2*2048*768*nc, bytes_accessed=2048*nc*2, transcendentals=0),
        compiler_params=pltpu.CompilerParams(dimension_semantics=("arbitrary",), vmem_limit_bytes=50*2**20), **kw)(*args)

NCH = 1
def solution(mesh):
    def f(h, w):
        n = 32
        H = lax.all_gather(h, ("dp", "tp"), axis=0, tiled=True)
        h3 = H.reshape(2048, 32, 20)
        z = jnp.zeros((2048, 32, 4), jnp.bfloat16)
        h4 = jnp.concatenate([h3[:, :, 0:8].reshape(2048, 256), h3[:, :, 8:16].reshape(2048, 256),
             jnp.concatenate([h3[:, :, 16:], z], 2).reshape(2048, 256),
             jnp.concatenate([z, h3[:, :, 16:]], 2).reshape(2048, 256)], 1)
        nc = 8192 // NCH
        w3 = w.reshape(20, n, NCH, nc)
        y = None
        for c in range(NCH):
            x = w3[:, :, c]
            a1 = x[0:8].transpose(1, 0, 2); a2 = x[8:16].transpose(1, 0, 2)
            b = x[16:].reshape(4, n, 2, nc // 2).transpose(1, 2, 0, 3).reshape(n, 8, nc // 2)
            p = jnp.concatenate([a1, a2, b], 2)
            r = lax.all_to_all(p, ("dp", "tp"), 0, 0, tiled=True).reshape(256, nc * 5 // 2)
            y = chunk_mm(h4, r, y, c, nc)
        return y
    return jax.shard_map(f, mesh=mesh, in_specs=(P(("dp", "tp"), None), P(("dp", "tp"), None)),
        out_specs=P(None, ("dp", "tp")), check_vma=False)
```

```python
import functools

import jax
import jax.numpy as jnp
from jax import lax
from jax.experimental import pallas as pl
from jax.experimental.pallas import tpu as pltpu
from jax.sharding import PartitionSpec as P

MESH = pl.DeviceIdType.MESH
NZ, NP = 4, 8
N = NZ * NP
ROWS, BLK, D = 2048, 64, 640
KA = 16
KB = 4
COLS = 8192
WID = 2048
NCH = COLS // WID
NPRE = NCH - 1
LOOK = 2
TN = 256
TM = 512


def send_order():
    order = []
    for m in range(NP):
        order += [(2, m), (1, m), (3, m)]
        if m:
            order.append((0, m))
    return order


ORDER = send_order()


def product(hp_ref, ra, rb, m, n):
    a = jnp.dot(hp_ref[m, 0 : N * KA], ra[:, n], preferred_element_type=jnp.float32)
    b = jnp.dot(hp_ref[m, N * KA : D], rb[:, n], preferred_element_type=jnp.float32)
    return (a + b).astype(jnp.bfloat16)


def exchange(h_ref, w_ref, y0, y1, y2, hp_ref, ra_last, rb_last, ra, rb, rbp, hraw, bsrc,
             loc, hz_s, hz_r, hp_s, hp_r, a_s, a_r, b_s, b_r):
    i, j = lax.axis_index("dp"), lax.axis_index("tp")
    me = i * NP + j

    bcopy = pltpu.make_async_copy(w_ref.at[KA : KA + KB, :], bsrc, loc.at[0])
    bcopy.start()
    hown = pltpu.make_async_copy(h_ref, hraw.at[j, i], loc.at[1])
    hown.start()

    barrier = pltpu.get_barrier_semaphore()

    def peer(kz, kp):
        return {"dp": i ^ kz, "tp": j ^ kp}

    for kz, kp in ORDER:
        pl.semaphore_signal(barrier, inc=1, device_id=peer(kz, kp), device_id_type=MESH)
    pl.semaphore_wait(barrier, N - 1)

    def dst_a(c):
        return ra.at[c] if c < NPRE else ra_last

    def dst_b(c):
        return rb.at[c] if c < NPRE else rb_last

    def cols(dev, c):
        return pl.ds(pl.multiple_of(dev * COLS + c * WID, WID), WID)

    def rows_a():
        return pl.ds(pl.multiple_of(me * KA, KA), KA)

    def send_a(c):
        for kz, kp in ORDER:
            dev = (i ^ kz) * NP + (j ^ kp)
            pltpu.make_async_remote_copy(
                w_ref.at[0:KA, cols(dev, c)], dst_a(c).at[rows_a(), :],
                a_s.at[c], a_r.at[c], device_id=peer(kz, kp), device_id_type=MESH).start()
        pltpu.make_async_copy(w_ref.at[0:KA, cols(me, c)], dst_a(c).at[rows_a(), :], a_r.at[c]).start()

    def send_b(c):
        for kz, kp in ORDER:
            dev = (i ^ kz) * NP + (j ^ kp)
            pltpu.make_async_remote_copy(
                bsrc.at[:, cols(dev, c)], dst_b(c).at[me],
                b_s.at[c], b_r.at[c], device_id=peer(kz, kp), device_id_type=MESH).start()
        pltpu.make_async_copy(w_ref.at[KA : KA + KB, cols(me, c)], dst_b(c).at[me], b_r.at[c]).start()

    for kz in (2, 3, 1):
        pltpu.make_async_remote_copy(
            h_ref, hraw.at[j, i], hz_s, hz_r, device_id=peer(kz, 0), device_id_type=MESH).start()
    send_a(0)
    bcopy.wait()
    send_b(0)
    hown.wait()
    pltpu.make_async_copy(hraw.at[j, 0:3], hraw.at[j, 0:3], hz_r).wait()
    for kp in range(1, NP):
        pltpu.make_async_remote_copy(
            hraw.at[j], hraw.at[j], hp_s, hp_r, device_id=peer(0, kp), device_id_type=MESH).start()
    for c in range(1, LOOK):
        send_a(c)
        send_b(c)

    pltpu.make_async_copy(hraw.at[0 : NP - 1], hraw.at[0 : NP - 1], hp_r).wait()
    row = lax.broadcasted_iota(jnp.int32, (D, D), 0)
    col = lax.broadcasted_iota(jnp.int32, (D, D), 1)
    src = (row * 3277) >> 16
    r = row - src * (KA + KB)
    to = jnp.where(r < KA, src * KA + r, N * KA + src * KB + r - KA)
    perm = jnp.where(to == col, 1.0, 0.0).astype(jnp.bfloat16)
    for p in range(NP):
        x = hraw[p].reshape(NZ * BLK, D)
        x = jnp.dot(x, perm, preferred_element_type=jnp.float32).astype(jnp.bfloat16)
        for z in range(NZ):
            hp_ref[pl.ds((z * NP + p) * BLK, BLK), :] = x[z * BLK : (z + 1) * BLK]

    for c in range(NCH):
        if c + LOOK < NCH:
            send_a(c + LOOK)
            send_b(c + LOOK)
        pltpu.make_async_copy(dst_a(c), dst_a(c), a_r.at[c]).wait()
        pltpu.make_async_copy(dst_b(c), dst_b(c), b_r.at[c]).wait()
        if c < NPRE:
            rbp[...] = rb[c].reshape(N * KB, WID)

            @pl.loop(0, WID // TN)
            def _(t):
                n = pl.ds(pl.multiple_of(t * TN, TN), TN)

                @pl.loop(0, ROWS // TM)
                def _(u):
                    m = pl.ds(pl.multiple_of(u * TM, TM), TM)
                    (y0, y1, y2)[c][m, n] = product(hp_ref, ra.at[c], rbp, m, n)

    pltpu.make_async_copy(hraw.at[0, 0:3], hraw.at[0, 0:3], hz_s).wait()
    pltpu.make_async_copy(hraw.at[0 : NP - 1], hraw.at[0 : NP - 1], hp_s).wait()
    for c in range(NCH):
        part = ra_last.at[0 : (N - 1) * KA, :]
        pltpu.make_async_copy(part, part, a_s.at[c]).wait()
        part = rb_last.at[0 : N - 1]
        pltpu.make_async_copy(part, part, b_s.at[c]).wait()


def finish(y0, y1, y2, hp_ref, ra, rb, out_ref, rbp, ybuf, sem_pre, sem):
    copies = []
    for t, y in enumerate((y0, y1, y2)):
        c = pltpu.make_async_copy(y, out_ref.at[:, t * WID : (t + 1) * WID], sem_pre.at[t])
        c.start()
        copies.append(c)
    rbp[...] = rb[...].reshape(N * KB, WID)
    for t in range(WID // TN):
        n = pl.ds(t * TN, TN)

        @pl.loop(0, ROWS // TM)
        def _(u):
            m = pl.ds(pl.multiple_of(u * TM, TM), TM)
            ybuf[m, n] = product(hp_ref, ra, rbp, m, n)

        c = pltpu.make_async_copy(ybuf.at[:, n], out_ref.at[:, pl.ds(NPRE * WID + t * TN, TN)], sem.at[t])
        c.start()
        copies.append(c)
    for c in copies:
        c.wait()


def local_part(h, w):
    bf = jnp.bfloat16
    any_, vmem = pl.BlockSpec(memory_space=pl.ANY), pl.BlockSpec(memory_space=pltpu.VMEM)
    dma = pltpu.SemaphoreType.DMA
    *ys, hp, ra, rb = pl.pallas_call(
        exchange,
        out_shape=(*[pltpu.VMEM((ROWS, WID), bf)] * NPRE, pltpu.VMEM((ROWS, D), bf),
                   pltpu.VMEM((N * KA, WID), bf), pltpu.VMEM((N, KB, WID), bf)),
        in_specs=[any_, any_],
        out_specs=(vmem,) * (NPRE + 3),
        scratch_shapes=[
            pltpu.VMEM((NPRE, N * KA, WID), bf), pltpu.VMEM((NPRE, N, KB, WID), bf),
            pltpu.VMEM((N * KB, WID), bf), pltpu.VMEM((NP, NZ, BLK, D), bf), pltpu.VMEM((KB, N * COLS), bf),
            dma((2,)), dma, dma, dma, dma, dma((NCH,)), dma((NCH,)), dma((NCH,)), dma((NCH,)),
        ],
        compiler_params=pltpu.CompilerParams(
            collective_id=0, has_side_effects=True, vmem_limit_bytes=20 * 2**20),
        name="exchange",
    )(h, w)
    return pl.pallas_call(
        finish,
        out_shape=jax.ShapeDtypeStruct((ROWS, COLS), bf),
        in_specs=[vmem] * (NPRE + 3),
        out_specs=any_,
        scratch_shapes=[pltpu.VMEM((N * KB, WID), bf), pltpu.VMEM((ROWS, WID), bf), dma((8,)), dma((WID // TN,))],
        compiler_params=pltpu.CompilerParams(vmem_limit_bytes=20 * 2**20),
        name="finish",
    )(*ys, hp, ra, rb)


def solution(mesh):
    return jax.shard_map(
        local_part,
        mesh=mesh,
        in_specs=(P(("dp", "tp"), None), P(("dp", "tp"), None)),
        out_specs=P(None, ("dp", "tp")),
        check_vma=False,
    )
```

```python
import jax
import jax.numpy as jnp
from jax import lax
from jax.experimental import pallas as pl
from jax.experimental.pallas import tpu as pltpu
from jax.sharding import PartitionSpec as P

MESH = pl.DeviceIdType.MESH
NZ, NP = 4, 8
N = NZ * NP
ROWS, BLK, D = 2048, 64, 640
KA = 16
KB = 4
COLS = 8192
WIDS = (2560, 2560, 2048, 1024)
OFFS = tuple(sum(WIDS[:c]) for c in range(len(WIDS)))
NCH = len(WIDS)
NPRE = NCH - 1
LOOK = 3
TN = 256
TM = 512

MSEQ = (0, 2, 4, 3, 1, 6, 5, 7)
CROSS = [(kz, m) for m in MSEQ for kz in (2, 3)]
STAY = [(kz, m) for m in MSEQ for kz in (1, 0) if (kz, m) != (0, 0)]


def product(hp_ref, ra, rb, m, n):
    a = jnp.dot(hp_ref[m, 0 : N * KA], ra[:, n], preferred_element_type=jnp.float32)
    b = jnp.dot(hp_ref[m, N * KA : D], rb[:, n], preferred_element_type=jnp.float32)
    return (a + b).astype(jnp.bfloat16)


def exchange(h_ref, w_ref, *refs):
    ys, (hp_ref, ra_last, rb_last), refs = refs[:NPRE], refs[NPRE : NPRE + 3], refs[NPRE + 3 :]
    ras, rbs, rbps, refs = refs[:NPRE], refs[NPRE : 2 * NPRE], refs[2 * NPRE : 3 * NPRE], refs[3 * NPRE :]
    hraw, bsrc, loc, hz_s, hm_r, hn_r, hp_s, hp_r, a_s, a_r, b_s, b_r = refs
    ras, rbs = (*ras, ra_last), (*rbs, rb_last)
    i, j = lax.axis_index("dp"), lax.axis_index("tp")
    me = i * NP + j
    inner = jnp.logical_and(i >= 1, i <= 2)

    bcopy = pltpu.make_async_copy(w_ref.at[KA : KA + KB, :], bsrc, loc.at[0])
    bcopy.start()
    hown = pltpu.make_async_copy(h_ref, hraw.at[j, i], loc.at[1])
    hown.start()

    barrier = pltpu.get_barrier_semaphore()

    def peer(kz, kp):
        return {"dp": i ^ kz, "tp": j ^ kp}

    for kz, kp in CROSS + STAY:
        pl.semaphore_signal(barrier, inc=1, device_id=peer(kz, kp), device_id_type=MESH)
    pl.semaphore_wait(barrier, N - 1)

    def remote(src, dst, s, r, to):
        return pltpu.make_async_remote_copy(src, dst, s, r, device_id=to, device_id_type=MESH)

    def cols(dev, c):
        return pl.ds(pl.multiple_of(dev * COLS + OFFS[c], 256), WIDS[c])

    rows_a = pl.ds(pl.multiple_of(me * KA, KA), KA)

    def send_list(c, order):
        for kz, kp in order:
            dev = (i ^ kz) * NP + (j ^ kp)
            remote(w_ref.at[0:KA, cols(dev, c)], ras[c].at[rows_a, :], a_s.at[c], a_r.at[c], peer(kz, kp)).start()
            remote(bsrc.at[:, cols(dev, c)], rbs[c].at[me], b_s.at[c], b_r.at[c], peer(kz, kp)).start()

    def send(c):
        @pl.when(inner)
        def _():
            send_list(c, CROSS + STAY)

        @pl.when(jnp.logical_not(inner))
        def _():
            send_list(c, STAY + CROSS)

        pltpu.make_async_copy(w_ref.at[0:KA, cols(me, c)], ras[c].at[rows_a, :], a_r.at[c]).start()
        pltpu.make_async_copy(w_ref.at[KA : KA + KB, cols(me, c)], rbs[c].at[me], b_r.at[c]).start()

    mirror = {"dp": NZ - 1 - i, "tp": j}
    remote(h_ref, hraw.at[j, i], hz_s, hm_r, mirror).start()
    remote(h_ref, hraw.at[j, i], hz_s, hn_r, peer(1, 0)).start()
    bcopy.wait()
    send(0)
    got = hraw.at[j, NZ - 1 - i]
    pltpu.make_async_copy(got, got, hm_r).wait()
    remote(got, got, hz_s, hn_r, peer(1, 0)).start()
    hown.wait()
    pltpu.make_async_copy(hraw.at[j, 0:2], hraw.at[j, 0:2], hn_r).wait()
    for kp in range(1, NP):
        remote(hraw.at[j], hraw.at[j], hp_s, hp_r, peer(0, kp)).start()
    for c in range(1, LOOK):
        send(c)

    pltpu.make_async_copy(hraw.at[0 : NP - 1], hraw.at[0 : NP - 1], hp_r).wait()
    row = lax.broadcasted_iota(jnp.int32, (D, D), 0)
    col = lax.broadcasted_iota(jnp.int32, (D, D), 1)
    src = (row * 3277) >> 16
    r = row - src * (KA + KB)
    to = jnp.where(r < KA, src * KA + r, N * KA + src * KB + r - KA)
    perm = jnp.where(to == col, 1.0, 0.0).astype(jnp.bfloat16)
    for p in range(NP):
        x = hraw[p].reshape(NZ * BLK, D)
        x = jnp.dot(x, perm, preferred_element_type=jnp.float32).astype(jnp.bfloat16)
        for z in range(NZ):
            hp_ref[pl.ds((z * NP + p) * BLK, BLK), :] = x[z * BLK : (z + 1) * BLK]

    for c in range(NCH):
        pltpu.make_async_copy(ras[c], ras[c], a_r.at[c]).wait()
        pltpu.make_async_copy(rbs[c], rbs[c], b_r.at[c]).wait()
        if c + LOOK < NCH:
            send(c + LOOK)
        if c < NPRE:
            rbps[c][...] = rbs[c][...].reshape(N * KB, WIDS[c])

            @pl.loop(0, WIDS[c] // TN)
            def _(t):
                n = pl.ds(pl.multiple_of(t * TN, TN), TN)

                @pl.loop(0, ROWS // TM)
                def _(u):
                    m = pl.ds(pl.multiple_of(u * TM, TM), TM)
                    ys[c][m, n] = product(hp_ref, ras[c], rbps[c], m, n)

    pltpu.make_async_copy(hraw.at[0, 0:3], hraw.at[0, 0:3], hz_s).wait()
    pltpu.make_async_copy(hraw.at[0 : NP - 1], hraw.at[0 : NP - 1], hp_s).wait()
    for c in range(NCH):
        part = ras[c].at[0 : (N - 1) * KA, :]
        pltpu.make_async_copy(part, part, a_s.at[c]).wait()
        part = rbs[c].at[0 : N - 1]
        pltpu.make_async_copy(part, part, b_s.at[c]).wait()


def finish(*refs):
    ys, (hp_ref, ra, rb, out_ref, rbp, ybuf, sem_pre, sem) = refs[:NPRE], refs[NPRE:]
    copies = []
    for c, y in enumerate(ys):
        copy = pltpu.make_async_copy(y, out_ref.at[:, OFFS[c] : OFFS[c] + WIDS[c]], sem_pre.at[c])
        copy.start()
        copies.append(copy)
    rbp[...] = rb[...].reshape(N * KB, WIDS[-1])
    for t in range(WIDS[-1] // TN):
        n = pl.ds(t * TN, TN)

        @pl.loop(0, ROWS // TM)
        def _(u):
            m = pl.ds(pl.multiple_of(u * TM, TM), TM)
            ybuf[m, n] = product(hp_ref, ra, rbp, m, n)

        copy = pltpu.make_async_copy(ybuf.at[:, n], out_ref.at[:, pl.ds(OFFS[-1] + t * TN, TN)], sem.at[t])
        copy.start()
        copies.append(copy)
    for copy in copies:
        copy.wait()


def local_part(h, w):
    bf = jnp.bfloat16
    any_, vmem = pl.BlockSpec(memory_space=pl.ANY), pl.BlockSpec(memory_space=pltpu.VMEM)
    hbm = pl.BlockSpec(memory_space=pltpu.HBM)
    dma = pltpu.SemaphoreType.DMA
    last = WIDS[-1]
    passed = pl.pallas_call(
        exchange,
        out_shape=(*[pltpu.VMEM((ROWS, wid), bf) for wid in WIDS[:NPRE]], pltpu.VMEM((ROWS, D), bf),
                   pltpu.VMEM((N * KA, last), bf), pltpu.VMEM((N, KB, last), bf)),
        in_specs=[hbm, hbm],
        out_specs=(vmem,) * (NPRE + 3),
        scratch_shapes=[
            *[pltpu.VMEM((N * KA, wid), bf) for wid in WIDS[:NPRE]],
            *[pltpu.VMEM((N, KB, wid), bf) for wid in WIDS[:NPRE]],
            *[pltpu.VMEM((N * KB, wid), bf) for wid in WIDS[:NPRE]],
            pltpu.VMEM((NP, NZ, BLK, D), bf), pltpu.VMEM((KB, N * COLS), bf),
            dma((2,)), dma, dma, dma, dma, dma, dma((NCH,)), dma((NCH,)), dma((NCH,)), dma((NCH,)),
        ],
        compiler_params=pltpu.CompilerParams(
            collective_id=0, has_side_effects=True, vmem_limit_bytes=22 * 2**20),
        name="exchange",
    )(pltpu.with_memory_space_constraint(h, pltpu.HBM), w)
    return pl.pallas_call(
        finish,
        out_shape=jax.ShapeDtypeStruct((ROWS, COLS), bf),
        in_specs=[vmem] * (NPRE + 3),
        out_specs=any_,
        scratch_shapes=[pltpu.VMEM((N * KB, last), bf), pltpu.VMEM((ROWS, last), bf), dma((NPRE,)), dma((last // TN,))],
        compiler_params=pltpu.CompilerParams(vmem_limit_bytes=22 * 2**20),
        name="finish",
    )(*passed)


def solution(mesh):
    return jax.shard_map(
        local_part,
        mesh=mesh,
        in_specs=(P(("dp", "tp"), None), P(("dp", "tp"), None)),
        out_specs=P(None, ("dp", "tp")),
        check_vma=False,
    )
```

```python
import jax
import jax.numpy as jnp
from jax import lax
from jax.experimental import pallas as pl
from jax.experimental.pallas import tpu as pltpu
from jax.sharding import PartitionSpec as P

MESH = pl.DeviceIdType.MESH
NZ, NP = 4, 8
N = NZ * NP
ROWS, BLK, D = 2048, 64, 640
KA = 16
KB = 4
COLS = 8192
WIDS = (2560, 2560, 2048, 1024)
OFFS = tuple(sum(WIDS[:c]) for c in range(len(WIDS)))
NCH = len(WIDS)
NPRE = NCH - 1
LOOK = 3
TN = 256
TM = 512

MSEQ = (0, 2, 4, 3, 1, 6, 5, 7)
CROSS = [(kz, m) for m in MSEQ for kz in (2, 3)]
STAY = [(kz, m) for m in MSEQ for kz in (1, 0) if (kz, m) != (0, 0)]


def plane(kz):
    return [(kz, m) for m in MSEQ if (kz, m) != (0, 0)]


def product(hp_ref, ra, rb, m, n):
    a = jnp.dot(hp_ref[m, 0 : N * KA], ra[:, n], preferred_element_type=jnp.float32)
    b = jnp.dot(hp_ref[m, N * KA : D], rb[:, n], preferred_element_type=jnp.float32)
    return (a + b).astype(jnp.bfloat16)


def exchange(h_ref, w_ref, *refs):
    ys, (hp_ref, ra_last, rb_last), refs = refs[:NPRE], refs[NPRE : NPRE + 3], refs[NPRE + 3 :]
    ras, rbs, rbps, refs = refs[:NPRE], refs[NPRE : 2 * NPRE], refs[2 * NPRE : 3 * NPRE], refs[3 * NPRE :]
    hraw, bsrc, news, loc, hz_s, hm_r, hn_r, hp_s, hp_r, a_s, a_r, b_s, b_r = refs
    ras, rbs = (*ras, ra_last), (*rbs, rb_last)
    i, j = lax.axis_index("dp"), lax.axis_index("tp")
    me = i * NP + j
    inner = jnp.logical_and(i >= 1, i <= 2)

    bcopy = pltpu.make_async_copy(w_ref.at[KA : KA + KB, :], bsrc, loc.at[0])
    bcopy.start()
    hown = pltpu.make_async_copy(h_ref, hraw.at[j, i], loc.at[1])
    hown.start()

    barrier = pltpu.get_barrier_semaphore()

    def peer(kz, kp):
        return {"dp": i ^ kz, "tp": j ^ kp}

    def tell(sem, kz, kp=0):
        pl.semaphore_signal(sem, inc=1, device_id=peer(kz, kp), device_id_type=MESH)

    for kz, kp in plane(0):
        tell(barrier, kz, kp)

    @pl.when(inner)
    def _():
        tell(barrier, 3)
        tell(barrier, 1)

    pl.semaphore_wait(barrier, NP)

    def remote(src, dst, s, r, to):
        return pltpu.make_async_remote_copy(src, dst, s, r, device_id=to, device_id_type=MESH)

    def cols(dev, c):
        return pl.ds(pl.multiple_of(dev * COLS + OFFS[c], 256), WIDS[c])

    rows_a = pl.ds(pl.multiple_of(me * KA, KA), KA)

    def send_list(c, order):
        for kz, kp in order:
            dev = (i ^ kz) * NP + (j ^ kp)
            remote(w_ref.at[0:KA, cols(dev, c)], ras[c].at[rows_a, :], a_s.at[c], a_r.at[c], peer(kz, kp)).start()
            remote(bsrc.at[:, cols(dev, c)], rbs[c].at[me], b_s.at[c], b_r.at[c], peer(kz, kp)).start()

    def send(c):
        @pl.when(inner)
        def _():
            send_list(c, CROSS + STAY)

        @pl.when(jnp.logical_not(inner))
        def _():
            send_list(c, STAY + CROSS)

        own(c)

    def own(c):
        pltpu.make_async_copy(w_ref.at[0:KA, cols(me, c)], ras[c].at[rows_a, :], a_r.at[c]).start()
        pltpu.make_async_copy(w_ref.at[KA : KA + KB, cols(me, c)], rbs[c].at[me], b_r.at[c]).start()

    def hidden(kz, r):
        remote(h_ref, hraw.at[j, i], hz_s, r, peer(kz, 0)).start()

    @pl.when(inner)
    def _():
        tell(news.at[0], 3)
        hidden(3, hm_r)
        bcopy.wait()
        send_list(0, [(3, 0)])
        pl.semaphore_wait(news.at[0], 1)
        send_list(0, plane(3)[1:])
        pl.semaphore_wait(news.at[1], 1)
        tell(news.at[2], 3)
        hidden(1, hn_r)
        pl.semaphore_wait(news.at[2], 1)
        tell(news.at[3], 1)
        send_list(0, plane(2) + STAY)

    @pl.when(jnp.logical_not(inner))
    def _():
        tell(news.at[1], 1)
        hidden(1, hn_r)
        bcopy.wait()
        send_list(0, plane(0))
        pl.semaphore_wait(news.at[3], 1)
        hidden(3, hm_r)
        send_list(0, plane(1) + CROSS)

    own(0)
    got = hraw.at[j, NZ - 1 - i]
    pltpu.make_async_copy(got, got, hm_r).wait()
    remote(got, got, hz_s, hn_r, peer(1, 0)).start()
    hown.wait()
    pltpu.make_async_copy(hraw.at[j, 0:2], hraw.at[j, 0:2], hn_r).wait()
    for kp in range(1, NP):
        remote(hraw.at[j], hraw.at[j], hp_s, hp_r, peer(0, kp)).start()
    for c in range(1, LOOK):
        send(c)

    pltpu.make_async_copy(hraw.at[0 : NP - 1], hraw.at[0 : NP - 1], hp_r).wait()
    row = lax.broadcasted_iota(jnp.int32, (D, D), 0)
    col = lax.broadcasted_iota(jnp.int32, (D, D), 1)
    src = (row * 3277) >> 16
    r = row - src * (KA + KB)
    to = jnp.where(r < KA, src * KA + r, N * KA + src * KB + r - KA)
    perm = jnp.where(to == col, 1.0, 0.0).astype(jnp.bfloat16)
    for p in range(NP):
        x = hraw[p].reshape(NZ * BLK, D)
        x = jnp.dot(x, perm, preferred_element_type=jnp.float32).astype(jnp.bfloat16)
        for z in range(NZ):
            hp_ref[pl.ds((z * NP + p) * BLK, BLK), :] = x[z * BLK : (z + 1) * BLK]

    for c in range(NCH):
        pltpu.make_async_copy(ras[c], ras[c], a_r.at[c]).wait()
        pltpu.make_async_copy(rbs[c], rbs[c], b_r.at[c]).wait()
        if c + LOOK < NCH:
            send(c + LOOK)
        if c < NPRE:
            rbps[c][...] = rbs[c][...].reshape(N * KB, WIDS[c])

            @pl.loop(0, WIDS[c] // TN)
            def _(t):
                n = pl.ds(pl.multiple_of(t * TN, TN), TN)

                @pl.loop(0, ROWS // TM)
                def _(u):
                    m = pl.ds(pl.multiple_of(u * TM, TM), TM)
                    ys[c][m, n] = product(hp_ref, ras[c], rbps[c], m, n)

    pltpu.make_async_copy(hraw.at[0, 0:3], hraw.at[0, 0:3], hz_s).wait()
    pltpu.make_async_copy(hraw.at[0 : NP - 1], hraw.at[0 : NP - 1], hp_s).wait()
    for c in range(NCH):
        part = ras[c].at[0 : (N - 1) * KA, :]
        pltpu.make_async_copy(part, part, a_s.at[c]).wait()
        part = rbs[c].at[0 : N - 1]
        pltpu.make_async_copy(part, part, b_s.at[c]).wait()


def finish(*refs):
    ys, (hp_ref, ra, rb, out_ref, rbp, ybuf, sem_pre, sem) = refs[:NPRE], refs[NPRE:]
    copies = []

    def put(src, u, c, s):
        m = pl.ds(u * TM, TM)
        copy = pltpu.make_async_copy(src.at[m, :], out_ref.at[m, OFFS[c] : OFFS[c] + WIDS[c]], s)
        copy.start(priority=len(copies) % 2)
        copies.append(copy)

    for u in range(ROWS // TM):
        for c, y in enumerate(ys):
            put(y, u, c, sem_pre.at[c, u])
    rbp[...] = rb[...].reshape(N * KB, WIDS[-1])
    for u in range(ROWS // TM):
        m = pl.ds(u * TM, TM)

        @pl.loop(0, WIDS[-1] // TN)
        def _(t):
            n = pl.ds(pl.multiple_of(t * TN, TN), TN)
            ybuf[m, n] = product(hp_ref, ra, rbp, m, n)

        put(ybuf, u, NCH - 1, sem.at[u])
    for copy in copies:
        copy.wait()


def local_part(h, w):
    bf = jnp.bfloat16
    any_, vmem = pl.BlockSpec(memory_space=pl.ANY), pl.BlockSpec(memory_space=pltpu.VMEM)
    hbm = pl.BlockSpec(memory_space=pltpu.HBM)
    dma = pltpu.SemaphoreType.DMA
    last = WIDS[-1]
    passed = pl.pallas_call(
        exchange,
        out_shape=(*[pltpu.VMEM((ROWS, wid), bf) for wid in WIDS[:NPRE]], pltpu.VMEM((ROWS, D), bf),
                   pltpu.VMEM((N * KA, last), bf), pltpu.VMEM((N, KB, last), bf)),
        in_specs=[hbm, hbm],
        out_specs=(vmem,) * (NPRE + 3),
        scratch_shapes=[
            *[pltpu.VMEM((N * KA, wid), bf) for wid in WIDS[:NPRE]],
            *[pltpu.VMEM((N, KB, wid), bf) for wid in WIDS[:NPRE]],
            *[pltpu.VMEM((N * KB, wid), bf) for wid in WIDS[:NPRE]],
            pltpu.VMEM((NP, NZ, BLK, D), bf), pltpu.VMEM((KB, N * COLS), bf),
            pltpu.SemaphoreType.REGULAR((4,)), dma((2,)), dma, dma, dma, dma, dma, dma((NCH,)), dma((NCH,)), dma((NCH,)), dma((NCH,)),
        ],
        compiler_params=pltpu.CompilerParams(
            collective_id=0, has_side_effects=True, vmem_limit_bytes=22 * 2**20),
        name="exchange",
    )(pltpu.with_memory_space_constraint(h, pltpu.HBM), w)
    return pl.pallas_call(
        finish,
        out_shape=jax.ShapeDtypeStruct((ROWS, COLS), bf),
        in_specs=[vmem] * (NPRE + 3),
        out_specs=any_,
        scratch_shapes=[pltpu.VMEM((N * KB, last), bf), pltpu.VMEM((ROWS, last), bf), dma((NPRE, ROWS // TM)), dma((ROWS // TM,))],
        compiler_params=pltpu.CompilerParams(vmem_limit_bytes=22 * 2**20),
        name="finish",
    )(*passed)


def solution(mesh):
    return jax.shard_map(
        local_part,
        mesh=mesh,
        in_specs=(P(("dp", "tp"), None), P(("dp", "tp"), None)),
        out_specs=P(None, ("dp", "tp")),
        check_vma=False,
    )
```

```python
import jax
import jax.numpy as jnp
from jax import lax
from jax.experimental import pallas as pl
from jax.experimental.pallas import tpu as pltpu
from jax.sharding import PartitionSpec as P

MESH = pl.DeviceIdType.MESH
NZ, NP = 4, 8
N = NZ * NP
ROWS, BLK, D = 2048, 64, 640
KA = 16
KB = 4
COLS = 8192
WIDS = (2560, 2560, 2048, 1024)
OFFS = tuple(sum(WIDS[:c]) for c in range(len(WIDS)))
NCH = len(WIDS)
NPRE = NCH - 1
LOOK = 3
TN = 256
TM = 512

MSEQ = (0, 2, 4, 3, 1, 6, 5, 7)
CROSS = [(kz, m) for m in MSEQ for kz in (2, 3)]
STAY = [(kz, m) for m in MSEQ for kz in (1, 0) if (kz, m) != (0, 0)]


def plane(kz):
    return [(kz, m) for m in MSEQ if (kz, m) != (0, 0)]


def product(hp_ref, ra, rb, m, n):
    a = jnp.dot(hp_ref[m, 0 : N * KA], ra[:, n], preferred_element_type=jnp.float32)
    b = jnp.dot(hp_ref[m, N * KA : D], rb[:, n], preferred_element_type=jnp.float32)
    return (a + b).astype(jnp.bfloat16)


def exchange(h_ref, w_ref, *refs):
    ys, (hp_ref, ra_last, rb_last), refs = refs[:NPRE], refs[NPRE : NPRE + 3], refs[NPRE + 3 :]
    ras, rbs, rbps, refs = refs[:NPRE], refs[NPRE : 2 * NPRE], refs[2 * NPRE : 3 * NPRE], refs[3 * NPRE :]
    hraw, bsrc, news, loc, hz_s, hm_r, hn_r, hp_s, hp_r, a_s, a_r, b_s, b_r = refs
    ras, rbs = (*ras, ra_last), (*rbs, rb_last)
    i, j = lax.axis_index("dp"), lax.axis_index("tp")
    me = i * NP + j
    inner = jnp.logical_and(i >= 1, i <= 2)

    bcopy = pltpu.make_async_copy(w_ref.at[KA : KA + KB, :], bsrc, loc.at[0])
    bcopy.start()
    hown = pltpu.make_async_copy(h_ref, hraw.at[j, i], loc.at[1])
    hown.start()

    barrier = pltpu.get_barrier_semaphore()

    def peer(kz, kp):
        return {"dp": i ^ kz, "tp": j ^ kp}

    def tell(sem, kz, kp=0):
        pl.semaphore_signal(sem, inc=1, device_id=peer(kz, kp), device_id_type=MESH)

    for kz, kp in plane(0):
        tell(barrier, kz, kp)

    @pl.when(inner)
    def _():
        tell(barrier, 3)
        tell(barrier, 1)

    hown.wait()
    pl.semaphore_wait(barrier, NP)

    def remote(src, dst, s, r, to):
        return pltpu.make_async_remote_copy(src, dst, s, r, device_id=to, device_id_type=MESH)

    def cols(dev, c):
        return pl.ds(pl.multiple_of(dev * COLS + OFFS[c], 256), WIDS[c])

    rows_a = pl.ds(pl.multiple_of(me * KA, KA), KA)

    def send_list(c, order):
        for kz, kp in order:
            dev = (i ^ kz) * NP + (j ^ kp)
            remote(w_ref.at[0:KA, cols(dev, c)], ras[c].at[rows_a, :], a_s.at[c], a_r.at[c], peer(kz, kp)).start()
            remote(bsrc.at[:, cols(dev, c)], rbs[c].at[me], b_s.at[c], b_r.at[c], peer(kz, kp)).start()

    def send(c):
        if c >= 2:
            send_list(c, STAY + CROSS)
        else:
            @pl.when(inner)
            def _():
                send_list(c, CROSS + STAY)

            @pl.when(jnp.logical_not(inner))
            def _():
                send_list(c, STAY + CROSS)

        own(c)

    def own(c):
        pltpu.make_async_copy(w_ref.at[0:KA, cols(me, c)], ras[c].at[rows_a, :], a_r.at[c]).start()
        pltpu.make_async_copy(w_ref.at[KA : KA + KB, cols(me, c)], rbs[c].at[me], b_r.at[c]).start()

    def hidden(kz, r):
        remote(hraw.at[j, i], hraw.at[j, i], hz_s, r, peer(kz, 0)).start()

    @pl.when(inner)
    def _():
        tell(news.at[0], 3)
        hidden(3, hm_r)
        bcopy.wait()
        send_list(0, [(3, 0)])
        pl.semaphore_wait(news.at[0], 1)
        send_list(0, plane(3)[1:])
        pl.semaphore_wait(news.at[1], 1)
        tell(news.at[2], 3)
        hidden(1, hn_r)
        pl.semaphore_wait(news.at[2], 1)
        tell(news.at[3], 1)
        send_list(0, plane(2) + STAY)

    @pl.when(jnp.logical_not(inner))
    def _():
        tell(news.at[1], 1)
        hidden(1, hn_r)
        bcopy.wait()
        send_list(0, plane(0))
        pl.semaphore_wait(news.at[3], 1)
        hidden(3, hm_r)
        send_list(0, plane(1) + CROSS)

    own(0)
    got = hraw.at[j, NZ - 1 - i]
    pltpu.make_async_copy(got, got, hm_r).wait()
    remote(got, got, hz_s, hn_r, peer(1, 0)).start()
    pltpu.make_async_copy(hraw.at[j, 0:2], hraw.at[j, 0:2], hn_r).wait()
    for kp in range(1, NP):
        remote(hraw.at[j], hraw.at[j], hp_s, hp_r, peer(0, kp)).start()
    for c in range(1, LOOK):
        send(c)

    pltpu.make_async_copy(hraw.at[0 : NP - 1], hraw.at[0 : NP - 1], hp_r).wait()
    row = lax.broadcasted_iota(jnp.int32, (D, D), 0)
    col = lax.broadcasted_iota(jnp.int32, (D, D), 1)
    src = (row * 3277) >> 16
    r = row - src * (KA + KB)
    to = jnp.where(r < KA, src * KA + r, N * KA + src * KB + r - KA)
    perm = jnp.where(to == col, 1.0, 0.0).astype(jnp.bfloat16)
    for p in range(NP):
        x = hraw[p].reshape(NZ * BLK, D)
        x = jnp.dot(x, perm, preferred_element_type=jnp.float32).astype(jnp.bfloat16)
        for z in range(NZ):
            hp_ref[pl.ds((z * NP + p) * BLK, BLK), :] = x[z * BLK : (z + 1) * BLK]

    for c in range(NCH):
        pltpu.make_async_copy(ras[c], ras[c], a_r.at[c]).wait()
        pltpu.make_async_copy(rbs[c], rbs[c], b_r.at[c]).wait()
        if c + LOOK < NCH:
            send(c + LOOK)
        if c < NPRE:
            rbps[c][...] = rbs[c][...].reshape(N * KB, WIDS[c])

            @pl.loop(0, WIDS[c] // TN)
            def _(t):
                n = pl.ds(pl.multiple_of(t * TN, TN), TN)

                @pl.loop(0, ROWS // TM)
                def _(u):
                    m = pl.ds(pl.multiple_of(u * TM, TM), TM)
                    ys[c][m, n] = product(hp_ref, ras[c], rbps[c], m, n)

    pltpu.make_async_copy(hraw.at[0, 0:3], hraw.at[0, 0:3], hz_s).wait()
    pltpu.make_async_copy(hraw.at[0 : NP - 1], hraw.at[0 : NP - 1], hp_s).wait()
    for c in range(NCH):
        part = ras[c].at[0 : (N - 1) * KA, :]
        pltpu.make_async_copy(part, part, a_s.at[c]).wait()
        part = rbs[c].at[0 : N - 1]
        pltpu.make_async_copy(part, part, b_s.at[c]).wait()


def finish(*refs):
    ys, (hp_ref, ra, rb, out_ref, rbp, ybuf, sem_pre, sem) = refs[:NPRE], refs[NPRE:]
    copies = []

    def put(src, u, c, s):
        m = pl.ds(u * TM, TM)
        copy = pltpu.make_async_copy(src.at[m, :], out_ref.at[m, OFFS[c] : OFFS[c] + WIDS[c]], s)
        copy.start(priority=len(copies) % 2)
        copies.append(copy)

    for u in range(ROWS // TM):
        for c, y in enumerate(ys):
            put(y, u, c, sem_pre.at[c, u])
    rbp[...] = rb[...].reshape(N * KB, WIDS[-1])
    for u in range(ROWS // TM):
        m = pl.ds(u * TM, TM)

        @pl.loop(0, WIDS[-1] // TN)
        def _(t):
            n = pl.ds(pl.multiple_of(t * TN, TN), TN)
            ybuf[m, n] = product(hp_ref, ra, rbp, m, n)

        put(ybuf, u, NCH - 1, sem.at[u])
    for copy in copies:
        copy.wait()


def local_part(h, w):
    bf = jnp.bfloat16
    any_, vmem = pl.BlockSpec(memory_space=pl.ANY), pl.BlockSpec(memory_space=pltpu.VMEM)
    hbm = pl.BlockSpec(memory_space=pltpu.HBM)
    dma = pltpu.SemaphoreType.DMA
    last = WIDS[-1]
    passed = pl.pallas_call(
        exchange,
        out_shape=(*[pltpu.VMEM((ROWS, wid), bf) for wid in WIDS[:NPRE]], pltpu.VMEM((ROWS, D), bf),
                   pltpu.VMEM((N * KA, last), bf), pltpu.VMEM((N, KB, last), bf)),
        in_specs=[hbm, hbm],
        out_specs=(vmem,) * (NPRE + 3),
        scratch_shapes=[
            *[pltpu.VMEM((N * KA, wid), bf) for wid in WIDS[:NPRE]],
            *[pltpu.VMEM((N, KB, wid), bf) for wid in WIDS[:NPRE]],
            *[pltpu.VMEM((N * KB, wid), bf) for wid in WIDS[:NPRE]],
            pltpu.VMEM((NP, NZ, BLK, D), bf), pltpu.VMEM((KB, N * COLS), bf),
            pltpu.SemaphoreType.REGULAR((4,)), dma((2,)), dma, dma, dma, dma, dma, dma((NCH,)), dma((NCH,)), dma((NCH,)), dma((NCH,)),
        ],
        compiler_params=pltpu.CompilerParams(
            collective_id=0, has_side_effects=True, vmem_limit_bytes=22 * 2**20),
        name="exchange",
    )(pltpu.with_memory_space_constraint(h, pltpu.HBM), w)
    return pl.pallas_call(
        finish,
        out_shape=jax.ShapeDtypeStruct((ROWS, COLS), bf),
        in_specs=[vmem] * (NPRE + 3),
        out_specs=any_,
        scratch_shapes=[pltpu.VMEM((N * KB, last), bf), pltpu.VMEM((ROWS, last), bf), dma((NPRE, ROWS // TM)), dma((ROWS // TM,))],
        compiler_params=pltpu.CompilerParams(vmem_limit_bytes=22 * 2**20),
        name="finish",
    )(*passed)


def solution(mesh):
    return jax.shard_map(
        local_part,
        mesh=mesh,
        in_specs=(P(("dp", "tp"), None), P(("dp", "tp"), None)),
        out_specs=P(None, ("dp", "tp")),
        check_vma=False,
    )
```

```python
import jax
import jax.numpy as jnp
from jax import lax
from jax.experimental import pallas as pl
from jax.experimental.pallas import tpu as pltpu
from jax.sharding import PartitionSpec as P

MESH = pl.DeviceIdType.MESH
NZ, NP = 4, 8
N = NZ * NP
ROWS, BLK, D = 2048, 64, 640
KA = 16
KB = 4
COLS = 8192
WIDS = (2560, 2560, 2048, 1024)
OFFS = tuple(sum(WIDS[:c]) for c in range(len(WIDS)))
NCH = len(WIDS)
NPRE = NCH - 1
LOOK = 3
TN = 256
TM = 512

MSEQ = (0, 2, 4, 3, 1, 6, 5, 7)
CROSS = [(kz, m) for m in MSEQ for kz in (2, 3)]
STAY = [(kz, m) for m in MSEQ for kz in (1, 0) if (kz, m) != (0, 0)]


def plane(kz):
    return [(kz, m) for m in MSEQ if (kz, m) != (0, 0)]


def product(hp_ref, ra, rb, m, n):
    a = jnp.dot(hp_ref[m, 0 : N * KA], ra[:, n], preferred_element_type=jnp.float32)
    b = jnp.dot(hp_ref[m, N * KA : D], rb[:, n], preferred_element_type=jnp.float32)
    return (a + b).astype(jnp.bfloat16)


def exchange(h_ref, w_ref, *refs):
    ys, (hp_ref, ra_last, rb_last), refs = refs[:NPRE], refs[NPRE : NPRE + 3], refs[NPRE + 3 :]
    ras, rbs, rbps, refs = refs[:NPRE], refs[NPRE : 2 * NPRE], refs[2 * NPRE : 3 * NPRE], refs[3 * NPRE :]
    hraw, bsrc, news, loc, hz_s, hm_r, hn_r, hp_s, hp_r, a_s, a_r, b_s, b_r = refs
    ras, rbs = (*ras, ra_last), (*rbs, rb_last)
    i, j = lax.axis_index("dp"), lax.axis_index("tp")
    me = i * NP + j
    inner = jnp.logical_and(i >= 1, i <= 2)

    bcopy = pltpu.make_async_copy(w_ref.at[KA : KA + KB, :], bsrc, loc.at[0])
    bcopy.start()
    hown = pltpu.make_async_copy(h_ref, hraw.at[j, i], loc.at[1])
    hown.start()

    barrier = pltpu.get_barrier_semaphore()

    def peer(kz, kp):
        return {"dp": i ^ kz, "tp": j ^ kp}

    def tell(sem, kz, kp=0):
        pl.semaphore_signal(sem, inc=1, device_id=peer(kz, kp), device_id_type=MESH)

    @pl.when(inner)
    def _():
        tell(barrier, 3)
        tell(barrier, 1)
        pl.semaphore_wait(barrier, 1)

    @pl.when(jnp.logical_not(inner))
    def _():
        for kz, kp in plane(0):
            tell(barrier, kz, kp)
        pl.semaphore_wait(barrier, NP)

    def remote(src, dst, s, r, to):
        return pltpu.make_async_remote_copy(src, dst, s, r, device_id=to, device_id_type=MESH)

    def cols(dev, c):
        return pl.ds(pl.multiple_of(dev * COLS + OFFS[c], 256), WIDS[c])

    rows_a = pl.ds(pl.multiple_of(me * KA, KA), KA)

    def send_a(c, kz, kp):
        dev = (i ^ kz) * NP + (j ^ kp)
        remote(w_ref.at[0:KA, cols(dev, c)], ras[c].at[rows_a, :], a_s.at[c], a_r.at[c], peer(kz, kp)).start()

    def send_b(c, kz, kp):
        dev = (i ^ kz) * NP + (j ^ kp)
        remote(bsrc.at[:, cols(dev, c)], rbs[c].at[me], b_s.at[c], b_r.at[c], peer(kz, kp)).start()

    def send_list(c, order):
        for kz, kp in order:
            send_a(c, kz, kp)
            send_b(c, kz, kp)

    def send(c):
        @pl.when(inner)
        def _():
            send_list(c, [k for k in CROSS if c >= LOOK or k != (3, 0)] + STAY)

        @pl.when(jnp.logical_not(inner))
        def _():
            send_list(c, STAY + CROSS)

        own(c)

    def own(c):
        pltpu.make_async_copy(w_ref.at[0:KA, cols(me, c)], ras[c].at[rows_a, :], a_r.at[c]).start()
        pltpu.make_async_copy(w_ref.at[KA : KA + KB, cols(me, c)], rbs[c].at[me], b_r.at[c]).start()

    def hidden(kz, r):
        remote(h_ref, hraw.at[j, i], hz_s, r, peer(kz, 0)).start()

    @pl.when(inner)
    def _():
        hidden(3, hm_r)
        for c in range(LOOK):
            send_a(c, 3, 0)
        bcopy.wait()
        for c in range(LOOK):
            send_b(c, 3, 0)
        pl.semaphore_wait(news.at[1], 1)
        tell(news.at[2], 3)
        hidden(1, hn_r)
        pl.semaphore_wait(news.at[2], 1)
        tell(news.at[3], 1)
        send_list(0, plane(3)[1:] + plane(2) + STAY)

    @pl.when(jnp.logical_not(inner))
    def _():
        for kz, kp in plane(0):
            tell(news.at[0], kz, kp)
        hidden(1, hn_r)
        bcopy.wait()
        send_list(0, plane(0))
        pl.semaphore_wait(news.at[0], NP - 1)
        tell(news.at[1], 1)
        send_list(0, plane(1))
        pl.semaphore_wait(news.at[3], 1)
        hidden(3, hm_r)
        send_list(0, CROSS)

    own(0)
    got = hraw.at[j, NZ - 1 - i]
    pltpu.make_async_copy(got, got, hm_r).wait()
    remote(got, got, hz_s, hn_r, peer(1, 0)).start()
    hown.wait()
    pltpu.make_async_copy(hraw.at[j, 0:2], hraw.at[j, 0:2], hn_r).wait()
    for kp in range(1, NP):
        remote(hraw.at[j], hraw.at[j], hp_s, hp_r, peer(0, kp)).start()
    for c in range(1, LOOK):
        send(c)

    pltpu.make_async_copy(hraw.at[0 : NP - 1], hraw.at[0 : NP - 1], hp_r).wait()
    row = lax.broadcasted_iota(jnp.int32, (D, D), 0)
    col = lax.broadcasted_iota(jnp.int32, (D, D), 1)
    src = (row * 3277) >> 16
    r = row - src * (KA + KB)
    to = jnp.where(r < KA, src * KA + r, N * KA + src * KB + r - KA)
    perm = jnp.where(to == col, 1.0, 0.0).astype(jnp.bfloat16)
    for p in range(NP):
        x = hraw[p].reshape(NZ * BLK, D)
        x = jnp.dot(x, perm, preferred_element_type=jnp.float32).astype(jnp.bfloat16)
        for z in range(NZ):
            hp_ref[pl.ds((z * NP + p) * BLK, BLK), :] = x[z * BLK : (z + 1) * BLK]

    for c in range(NCH):
        pltpu.make_async_copy(ras[c], ras[c], a_r.at[c]).wait()
        pltpu.make_async_copy(rbs[c], rbs[c], b_r.at[c]).wait()
        if c + LOOK < NCH:
            send(c + LOOK)
        if c < NPRE:
            rbps[c][...] = rbs[c][...].reshape(N * KB, WIDS[c])

            @pl.loop(0, WIDS[c] // TN)
            def _(t):
                n = pl.ds(pl.multiple_of(t * TN, TN), TN)

                @pl.loop(0, ROWS // TM)
                def _(u):
                    m = pl.ds(pl.multiple_of(u * TM, TM), TM)
                    ys[c][m, n] = product(hp_ref, ras[c], rbps[c], m, n)

    pltpu.make_async_copy(hraw.at[0, 0:3], hraw.at[0, 0:3], hz_s).wait()
    pltpu.make_async_copy(hraw.at[0 : NP - 1], hraw.at[0 : NP - 1], hp_s).wait()
    for c in range(NCH):
        part = ras[c].at[0 : (N - 1) * KA, :]
        pltpu.make_async_copy(part, part, a_s.at[c]).wait()
        part = rbs[c].at[0 : N - 1]
        pltpu.make_async_copy(part, part, b_s.at[c]).wait()


def finish(*refs):
    ys, (hp_ref, ra, rb, out_ref, rbp, ybuf, sem_pre, sem) = refs[:NPRE], refs[NPRE:]
    copies = []

    def put(src, u, c, s):
        m = pl.ds(u * TM, TM)
        copy = pltpu.make_async_copy(src.at[m, :], out_ref.at[m, OFFS[c] : OFFS[c] + WIDS[c]], s)
        copy.start(priority=len(copies) % 2)
        copies.append(copy)

    for u in range(ROWS // TM):
        for c, y in enumerate(ys):
            put(y, u, c, sem_pre.at[c, u])
    rbp[...] = rb[...].reshape(N * KB, WIDS[-1])
    for u in range(ROWS // TM):
        m = pl.ds(u * TM, TM)

        @pl.loop(0, WIDS[-1] // TN)
        def _(t):
            n = pl.ds(pl.multiple_of(t * TN, TN), TN)
            ybuf[m, n] = product(hp_ref, ra, rbp, m, n)

        put(ybuf, u, NCH - 1, sem.at[u])
    for copy in copies:
        copy.wait()


def local_part(h, w):
    bf = jnp.bfloat16
    any_, vmem = pl.BlockSpec(memory_space=pl.ANY), pl.BlockSpec(memory_space=pltpu.VMEM)
    hbm = pl.BlockSpec(memory_space=pltpu.HBM)
    dma = pltpu.SemaphoreType.DMA
    last = WIDS[-1]
    passed = pl.pallas_call(
        exchange,
        out_shape=(*[pltpu.VMEM((ROWS, wid), bf) for wid in WIDS[:NPRE]], pltpu.VMEM((ROWS, D), bf),
                   pltpu.VMEM((N * KA, last), bf), pltpu.VMEM((N, KB, last), bf)),
        in_specs=[hbm, hbm],
        out_specs=(vmem,) * (NPRE + 3),
        scratch_shapes=[
            *[pltpu.VMEM((N * KA, wid), bf) for wid in WIDS[:NPRE]],
            *[pltpu.VMEM((N, KB, wid), bf) for wid in WIDS[:NPRE]],
            *[pltpu.VMEM((N * KB, wid), bf) for wid in WIDS[:NPRE]],
            pltpu.VMEM((NP, NZ, BLK, D), bf), pltpu.VMEM((KB, N * COLS), bf),
            pltpu.SemaphoreType.REGULAR((4,)), dma((2,)), dma, dma, dma, dma, dma, dma((NCH,)), dma((NCH,)), dma((NCH,)), dma((NCH,)),
        ],
        compiler_params=pltpu.CompilerParams(
            collective_id=0, has_side_effects=True, vmem_limit_bytes=22 * 2**20),
        name="exchange",
    )(pltpu.with_memory_space_constraint(h, pltpu.HBM), w)
    return pl.pallas_call(
        finish,
        out_shape=jax.ShapeDtypeStruct((ROWS, COLS), bf),
        in_specs=[vmem] * (NPRE + 3),
        out_specs=any_,
        scratch_shapes=[pltpu.VMEM((N * KB, last), bf), pltpu.VMEM((ROWS, last), bf), dma((NPRE, ROWS // TM)), dma((ROWS // TM,))],
        compiler_params=pltpu.CompilerParams(vmem_limit_bytes=22 * 2**20),
        name="finish",
    )(*passed)


def solution(mesh):
    return jax.shard_map(
        local_part,
        mesh=mesh,
        in_specs=(P(("dp", "tp"), None), P(("dp", "tp"), None)),
        out_specs=P(None, ("dp", "tp")),
        check_vma=False,
    )
```

```python
import jax
import jax.numpy as jnp
from jax import lax
from jax.experimental import pallas as pl
from jax.experimental.pallas import tpu as pltpu
from jax.sharding import PartitionSpec as P

MESH = pl.DeviceIdType.MESH
NZ, NP = 4, 8
N = NZ * NP
ROWS, BLK, D = 2048, 64, 640
KA = 16
KB = 4
COLS = 8192
WIDS = (2304, 2048, 1536, 1024, 512, 512, 256)
OFFS = tuple(sum(WIDS[:c]) for c in range(len(WIDS)))
NCH = len(WIDS)
NPRE = 5
NLATE = NCH - NPRE
LOOK = 3
TN = 256
TM = 512

MSEQ = (0, 2, 4, 3, 1, 6, 5, 7)
CROSS = [(kz, m) for m in MSEQ for kz in (2, 3)]
STAY = [(kz, m) for m in MSEQ for kz in (1, 0) if (kz, m) != (0, 0)]


def plane(kz):
    return [(kz, m) for m in MSEQ if (kz, m) != (0, 0)]


def product(hp_ref, ra, rb, m, n):
    a = jnp.dot(hp_ref[m, 0 : N * KA], ra[:, n], preferred_element_type=jnp.float32)
    b = jnp.dot(hp_ref[m, N * KA : D], rb[:, n], preferred_element_type=jnp.float32)
    return (a + b).astype(jnp.bfloat16)


def exchange(h_ref, w_ref, *refs):
    ys, hp_ref, refs = refs[:NPRE], refs[NPRE], refs[NPRE + 1 :]
    late, refs = refs[: 2 * NLATE], refs[2 * NLATE :]
    ras, rbs, rbps, refs = refs[:NPRE], refs[NPRE : 2 * NPRE], refs[2 * NPRE : 3 * NPRE], refs[3 * NPRE :]
    hraw, bsrc, news, loc, hz_s, hm_r, hn_r, hp_s, hp_r, a_s, a_r, b_s, b_r = refs
    ras, rbs = (*ras, *late[:NLATE]), (*rbs, *late[NLATE:])
    i, j = lax.axis_index("dp"), lax.axis_index("tp")
    me = i * NP + j
    inner = jnp.logical_and(i >= 1, i <= 2)

    bcopy = pltpu.make_async_copy(w_ref.at[KA : KA + KB, :], bsrc, loc.at[0])
    bcopy.start()
    hown = pltpu.make_async_copy(h_ref, hraw.at[j, i], loc.at[1])
    hown.start()

    barrier = pltpu.get_barrier_semaphore()

    def peer(kz, kp):
        return {"dp": i ^ kz, "tp": j ^ kp}

    def tell(sem, kz, kp=0):
        pl.semaphore_signal(sem, inc=1, device_id=peer(kz, kp), device_id_type=MESH)

    @pl.when(inner)
    def _():
        tell(barrier, 3)
        tell(barrier, 1)
        pl.semaphore_wait(barrier, 1)

    @pl.when(jnp.logical_not(inner))
    def _():
        for kz, kp in plane(0):
            tell(barrier, kz, kp)
        pl.semaphore_wait(barrier, NP)

    def remote(src, dst, s, r, to):
        return pltpu.make_async_remote_copy(src, dst, s, r, device_id=to, device_id_type=MESH)

    def cols(dev, c):
        return pl.ds(pl.multiple_of(dev * COLS + OFFS[c], 256), WIDS[c])

    rows_a = pl.ds(pl.multiple_of(me * KA, KA), KA)

    def send_a(c, kz, kp):
        dev = (i ^ kz) * NP + (j ^ kp)
        remote(w_ref.at[0:KA, cols(dev, c)], ras[c].at[rows_a, :], a_s.at[c], a_r.at[c], peer(kz, kp)).start()

    def send_b(c, kz, kp):
        dev = (i ^ kz) * NP + (j ^ kp)
        remote(bsrc.at[:, cols(dev, c)], rbs[c].at[me], b_s.at[c], b_r.at[c], peer(kz, kp)).start()

    def send_list(c, order):
        for kz, kp in order:
            send_a(c, kz, kp)
            send_b(c, kz, kp)

    def send(c):
        @pl.when(inner)
        def _():
            send_list(c, [k for k in CROSS if c >= LOOK or k != (3, 0)] + STAY)

        @pl.when(jnp.logical_not(inner))
        def _():
            send_list(c, STAY + CROSS)

        own(c)

    def own(c):
        pltpu.make_async_copy(w_ref.at[0:KA, cols(me, c)], ras[c].at[rows_a, :], a_r.at[c]).start()
        pltpu.make_async_copy(w_ref.at[KA : KA + KB, cols(me, c)], rbs[c].at[me], b_r.at[c]).start()

    def hidden(kz, r):
        remote(h_ref, hraw.at[j, i], hz_s, r, peer(kz, 0)).start()

    @pl.when(inner)
    def _():
        hidden(3, hm_r)
        for c in range(LOOK):
            send_a(c, 3, 0)
        bcopy.wait()
        for c in range(LOOK):
            send_b(c, 3, 0)
        pl.semaphore_wait(news.at[1], 1)
        tell(news.at[2], 3)
        hidden(1, hn_r)
        pl.semaphore_wait(news.at[2], 1)
        tell(news.at[3], 1)
        send_list(0, plane(3)[1:] + plane(2) + STAY)

    @pl.when(jnp.logical_not(inner))
    def _():
        for kz, kp in plane(0):
            tell(news.at[0], kz, kp)
        hidden(1, hn_r)
        bcopy.wait()
        send_list(0, plane(0))
        pl.semaphore_wait(news.at[0], NP - 1)
        tell(news.at[1], 1)
        send_list(0, plane(1))
        pl.semaphore_wait(news.at[3], 1)
        hidden(3, hm_r)
        send_list(0, CROSS)

    own(0)
    got = hraw.at[j, NZ - 1 - i]
    pltpu.make_async_copy(got, got, hm_r).wait()
    remote(got, got, hz_s, hn_r, peer(1, 0)).start()
    hown.wait()
    pltpu.make_async_copy(hraw.at[j, 0:2], hraw.at[j, 0:2], hn_r).wait()
    for kp in range(1, NP):
        remote(hraw.at[j], hraw.at[j], hp_s, hp_r, peer(0, kp)).start()
    for c in range(1, LOOK):
        send(c)

    pltpu.make_async_copy(hraw.at[0 : NP - 1], hraw.at[0 : NP - 1], hp_r).wait()
    row = lax.broadcasted_iota(jnp.int32, (D, D), 0)
    col = lax.broadcasted_iota(jnp.int32, (D, D), 1)
    src = (row * 3277) >> 16
    r = row - src * (KA + KB)
    to = jnp.where(r < KA, src * KA + r, N * KA + src * KB + r - KA)
    perm = jnp.where(to == col, 1.0, 0.0).astype(jnp.bfloat16)
    for p in range(NP):
        x = hraw[p].reshape(NZ * BLK, D)
        x = jnp.dot(x, perm, preferred_element_type=jnp.float32).astype(jnp.bfloat16)
        for z in range(NZ):
            hp_ref[pl.ds((z * NP + p) * BLK, BLK), :] = x[z * BLK : (z + 1) * BLK]

    for c in range(NCH):
        pltpu.make_async_copy(ras[c], ras[c], a_r.at[c]).wait()
        pltpu.make_async_copy(rbs[c], rbs[c], b_r.at[c]).wait()
        if c + LOOK < NCH:
            send(c + LOOK)
        if c < NPRE:
            rbps[c][...] = rbs[c][...].reshape(N * KB, WIDS[c])

            @pl.loop(0, WIDS[c] // TN)
            def _(t):
                n = pl.ds(pl.multiple_of(t * TN, TN), TN)

                @pl.loop(0, ROWS // TM)
                def _(u):
                    m = pl.ds(pl.multiple_of(u * TM, TM), TM)
                    ys[c][m, n] = product(hp_ref, ras[c], rbps[c], m, n)

    pltpu.make_async_copy(hraw.at[0, 0:3], hraw.at[0, 0:3], hz_s).wait()
    pltpu.make_async_copy(hraw.at[0 : NP - 1], hraw.at[0 : NP - 1], hp_s).wait()
    for c in range(NCH):
        part = ras[c].at[0 : (N - 1) * KA, :]
        pltpu.make_async_copy(part, part, a_s.at[c]).wait()
        part = rbs[c].at[0 : N - 1]
        pltpu.make_async_copy(part, part, b_s.at[c]).wait()


def finish(*refs):
    ys, hp_ref, refs = refs[:NPRE], refs[NPRE], refs[NPRE + 1 :]
    ras, rbs, out_ref, refs = refs[:NLATE], refs[NLATE : 2 * NLATE], refs[2 * NLATE], refs[2 * NLATE + 1 :]
    rbps, (ybuf, sem_pre, sem) = refs[:NLATE], refs[NLATE:]
    copies = []

    def put(src, u, off, wid, s):
        m = pl.ds(u * TM, TM)
        copy = pltpu.make_async_copy(src.at[m, :], out_ref.at[m, off : off + wid], s)
        copy.start(priority=len(copies) % 2)
        copies.append(copy)

    for u in range(ROWS // TM):
        for c, y in enumerate(ys):
            put(y, u, OFFS[c], WIDS[c], sem_pre.at[c, u])
    for c in range(NLATE):
        rbps[c][...] = rbs[c][...].reshape(N * KB, WIDS[NPRE + c])
    for u in range(ROWS // TM):
        m = pl.ds(u * TM, TM)
        for c in range(NLATE):
            for t in range(WIDS[NPRE + c] // TN):
                n = pl.ds(t * TN, TN)
                o = pl.ds(OFFS[NPRE + c] - OFFS[NPRE] + t * TN, TN)
                ybuf[m, o] = product(hp_ref, ras[c], rbps[c], m, n)
        put(ybuf, u, OFFS[NPRE], COLS - OFFS[NPRE], sem.at[u])
    for copy in copies:
        copy.wait()


def local_part(h, w):
    bf = jnp.bfloat16
    any_, vmem = pl.BlockSpec(memory_space=pl.ANY), pl.BlockSpec(memory_space=pltpu.VMEM)
    hbm = pl.BlockSpec(memory_space=pltpu.HBM)
    dma = pltpu.SemaphoreType.DMA
    pre, late = WIDS[:NPRE], WIDS[NPRE:]
    passed = pl.pallas_call(
        exchange,
        out_shape=(*[pltpu.VMEM((ROWS, wid), bf) for wid in pre], pltpu.VMEM((ROWS, D), bf),
                   *[pltpu.VMEM((N * KA, wid), bf) for wid in late], *[pltpu.VMEM((N, KB, wid), bf) for wid in late]),
        in_specs=[hbm, hbm],
        out_specs=(vmem,) * (NPRE + 1 + 2 * NLATE),
        scratch_shapes=[
            *[pltpu.VMEM((N * KA, wid), bf) for wid in pre],
            *[pltpu.VMEM((N, KB, wid), bf) for wid in pre],
            *[pltpu.VMEM((N * KB, wid), bf) for wid in pre],
            pltpu.VMEM((NP, NZ, BLK, D), bf), pltpu.VMEM((KB, N * COLS), bf),
            pltpu.SemaphoreType.REGULAR((4,)), dma((2,)), dma, dma, dma, dma, dma,
            dma((NCH,)), dma((NCH,)), dma((NCH,)), dma((NCH,)),
        ],
        compiler_params=pltpu.CompilerParams(
            collective_id=0, has_side_effects=True, vmem_limit_bytes=19 * 2**20),
        name="exchange",
    )(pltpu.with_memory_space_constraint(h, pltpu.HBM), w)
    return pl.pallas_call(
        finish,
        out_shape=jax.ShapeDtypeStruct((ROWS, COLS), bf),
        in_specs=[vmem] * (NPRE + 1 + 2 * NLATE),
        out_specs=any_,
        scratch_shapes=[*[pltpu.VMEM((N * KB, wid), bf) for wid in late], pltpu.VMEM((ROWS, sum(late)), bf),
                        dma((NPRE, ROWS // TM)), dma((ROWS // TM,))],
        compiler_params=pltpu.CompilerParams(vmem_limit_bytes=19 * 2**20),
        name="finish",
    )(*passed)


def solution(mesh):
    return jax.shard_map(
        local_part,
        mesh=mesh,
        in_specs=(P(("dp", "tp"), None), P(("dp", "tp"), None)),
        out_specs=P(None, ("dp", "tp")),
        check_vma=False,
    )
```

```python
import jax
import jax.numpy as jnp
from jax import lax
from jax.experimental import pallas as pl
from jax.experimental.pallas import tpu as pltpu
from jax.sharding import PartitionSpec as P

MESH = pl.DeviceIdType.MESH
NZ, NP = 4, 8
N = NZ * NP
ROWS, BLK, D = 2048, 64, 640
KA = 16
KB = 4
COLS = 8192
WIDS = (3328, 3328, 1536)
OFFS = tuple(sum(WIDS[:c]) for c in range(len(WIDS)))
NCH = len(WIDS)
NPRE = NCH - 1
LOOK = 3
TN = 256
TM = 512

MSEQ = (0, 2, 4, 3, 1, 6, 5, 7)
CROSS = [(kz, m) for m in MSEQ for kz in (2, 3)]
STAY = [(kz, m) for m in MSEQ for kz in (1, 0) if (kz, m) != (0, 0)]


def plane(kz):
    return [(kz, m) for m in MSEQ if (kz, m) != (0, 0)]


def product(hp_ref, ra, rb, m, n):
    a = jnp.dot(hp_ref[m, 0 : N * KA], ra[:, n], preferred_element_type=jnp.float32)
    b = jnp.dot(hp_ref[m, N * KA : D], rb[:, n], preferred_element_type=jnp.float32)
    return (a + b).astype(jnp.bfloat16)


def exchange(h_ref, w_ref, *refs):
    ys, (hp_ref, ra_last, rb), refs = refs[:NPRE], refs[NPRE : NPRE + 3], refs[NPRE + 3 :]
    ras, rbps, refs = refs[:NPRE], refs[NPRE : 2 * NPRE], refs[2 * NPRE :]
    hraw, bsrc, news, loc, hz_s, hm_r, hn_r, hp_s, hp_r, a_s, a_r, b_s, b_r = refs
    ras = (*ras, ra_last)
    i, j = lax.axis_index("dp"), lax.axis_index("tp")
    me = i * NP + j
    inner = jnp.logical_and(i >= 1, i <= 2)

    bcopy = pltpu.make_async_copy(w_ref.at[KA : KA + KB, :], bsrc, loc.at[0])
    bcopy.start()
    hown = pltpu.make_async_copy(h_ref, hraw.at[j, i], loc.at[1])
    hown.start()

    barrier = pltpu.get_barrier_semaphore()

    def peer(kz, kp):
        return {"dp": i ^ kz, "tp": j ^ kp}

    def tell(sem, kz, kp=0):
        pl.semaphore_signal(sem, inc=1, device_id=peer(kz, kp), device_id_type=MESH)

    @pl.when(inner)
    def _():
        tell(barrier, 3)
        tell(barrier, 1)
        pl.semaphore_wait(barrier, 1)

    @pl.when(jnp.logical_not(inner))
    def _():
        for kz, kp in plane(0):
            tell(barrier, kz, kp)
        pl.semaphore_wait(barrier, NP)

    def remote(src, dst, s, r, to):
        return pltpu.make_async_remote_copy(src, dst, s, r, device_id=to, device_id_type=MESH)

    def cols(dev, c):
        return pl.ds(pl.multiple_of(dev * COLS + OFFS[c], 256), WIDS[c])

    rows_a = pl.ds(pl.multiple_of(me * KA, KA), KA)

    def send_a(c, kz, kp):
        dev = (i ^ kz) * NP + (j ^ kp)
        remote(w_ref.at[0:KA, cols(dev, c)], ras[c].at[rows_a, :], a_s.at[c], a_r.at[c], peer(kz, kp)).start()

    def send_b(kz, kp):
        dev = (i ^ kz) * NP + (j ^ kp)
        part = bsrc.at[:, pl.ds(pl.multiple_of(dev * COLS, COLS), COLS)]
        remote(part, rb.at[me], b_s, b_r, peer(kz, kp)).start()

    def send_list(c, order):
        for kz, kp in order:
            send_a(c, kz, kp)
            if c == 0:
                send_b(kz, kp)

    def send(c):
        @pl.when(inner)
        def _():
            send_list(c, [k for k in CROSS if c >= LOOK or k != (3, 0)] + STAY)

        @pl.when(jnp.logical_not(inner))
        def _():
            send_list(c, STAY + CROSS)

        own(c)

    def own(c):
        pltpu.make_async_copy(w_ref.at[0:KA, cols(me, c)], ras[c].at[rows_a, :], a_r.at[c]).start()
        if c == 0:
            mine = pl.ds(pl.multiple_of(me * COLS, COLS), COLS)
            pltpu.make_async_copy(w_ref.at[KA : KA + KB, mine], rb.at[me], b_r).start()

    def hidden(kz, r):
        remote(h_ref, hraw.at[j, i], hz_s, r, peer(kz, 0)).start()

    @pl.when(inner)
    def _():
        hidden(3, hm_r)
        for c in range(LOOK):
            send_a(c, 3, 0)
        bcopy.wait()
        send_b(3, 0)
        pl.semaphore_wait(news.at[1], 1)
        tell(news.at[2], 3)
        hidden(1, hn_r)
        pl.semaphore_wait(news.at[2], 1)
        tell(news.at[3], 1)
        send_list(0, plane(3)[1:] + plane(2) + STAY)

    @pl.when(jnp.logical_not(inner))
    def _():
        for kz, kp in plane(0):
            tell(news.at[0], kz, kp)
        hidden(1, hn_r)
        bcopy.wait()
        send_list(0, plane(0))
        pl.semaphore_wait(news.at[0], NP - 1)
        tell(news.at[1], 1)
        send_list(0, plane(1))
        pl.semaphore_wait(news.at[3], 1)
        hidden(3, hm_r)
        send_list(0, CROSS)

    own(0)
    got = hraw.at[j, NZ - 1 - i]
    pltpu.make_async_copy(got, got, hm_r).wait()
    remote(got, got, hz_s, hn_r, peer(1, 0)).start()
    hown.wait()
    pltpu.make_async_copy(hraw.at[j, 0:2], hraw.at[j, 0:2], hn_r).wait()
    for kp in range(1, NP):
        remote(hraw.at[j], hraw.at[j], hp_s, hp_r, peer(0, kp)).start()
    for c in range(1, LOOK):
        send(c)

    pltpu.make_async_copy(hraw.at[0 : NP - 1], hraw.at[0 : NP - 1], hp_r).wait()
    row = lax.broadcasted_iota(jnp.int32, (D, D), 0)
    col = lax.broadcasted_iota(jnp.int32, (D, D), 1)
    src = (row * 3277) >> 16
    r = row - src * (KA + KB)
    to = jnp.where(r < KA, src * KA + r, N * KA + src * KB + r - KA)
    perm = jnp.where(to == col, 1.0, 0.0).astype(jnp.bfloat16)
    for p in range(NP):
        x = hraw[p].reshape(NZ * BLK, D)
        x = jnp.dot(x, perm, preferred_element_type=jnp.float32).astype(jnp.bfloat16)
        for z in range(NZ):
            hp_ref[pl.ds((z * NP + p) * BLK, BLK), :] = x[z * BLK : (z + 1) * BLK]

    for c in range(NCH):
        pltpu.make_async_copy(ras[c], ras[c], a_r.at[c]).wait()
        if c == 0:
            pltpu.make_async_copy(rb, rb, b_r).wait()
        if c + LOOK < NCH:
            send(c + LOOK)
        if c < NPRE:
            rbps[c][...] = rb[:, :, OFFS[c] : OFFS[c] + WIDS[c]].reshape(N * KB, WIDS[c])

            @pl.loop(0, WIDS[c] // TN)
            def _(t):
                n = pl.ds(pl.multiple_of(t * TN, TN), TN)

                @pl.loop(0, ROWS // TM)
                def _(u):
                    m = pl.ds(pl.multiple_of(u * TM, TM), TM)
                    ys[c][m, n] = product(hp_ref, ras[c], rbps[c], m, n)

    pltpu.make_async_copy(hraw.at[0, 0:3], hraw.at[0, 0:3], hz_s).wait()
    pltpu.make_async_copy(hraw.at[0 : NP - 1], hraw.at[0 : NP - 1], hp_s).wait()
    for c in range(NCH):
        part = ras[c].at[0 : (N - 1) * KA, :]
        pltpu.make_async_copy(part, part, a_s.at[c]).wait()
    part = rb.at[0 : N - 1]
    pltpu.make_async_copy(part, part, b_s).wait()


def finish(*refs):
    ys, (hp_ref, ra, rb, out_ref, rbp, ybuf, sem_pre, sem) = refs[:NPRE], refs[NPRE:]
    copies = []

    def put(src, u, c, s):
        m = pl.ds(u * TM, TM)
        copy = pltpu.make_async_copy(src.at[m, :], out_ref.at[m, OFFS[c] : OFFS[c] + WIDS[c]], s)
        copy.start(priority=len(copies) % 2)
        copies.append(copy)

    for u in range(ROWS // TM):
        for c, y in enumerate(ys):
            put(y, u, c, sem_pre.at[c, u])
    rbp[...] = rb[:, :, OFFS[-1] :].reshape(N * KB, WIDS[-1])
    for u in range(ROWS // TM):
        m = pl.ds(u * TM, TM)

        @pl.loop(0, WIDS[-1] // TN)
        def _(t):
            n = pl.ds(pl.multiple_of(t * TN, TN), TN)
            ybuf[m, n] = product(hp_ref, ra, rbp, m, n)

        put(ybuf, u, NCH - 1, sem.at[u])
    for copy in copies:
        copy.wait()


def local_part(h, w):
    bf = jnp.bfloat16
    any_, vmem = pl.BlockSpec(memory_space=pl.ANY), pl.BlockSpec(memory_space=pltpu.VMEM)
    hbm = pl.BlockSpec(memory_space=pltpu.HBM)
    dma = pltpu.SemaphoreType.DMA
    last = WIDS[-1]
    passed = pl.pallas_call(
        exchange,
        out_shape=(*[pltpu.VMEM((ROWS, wid), bf) for wid in WIDS[:NPRE]], pltpu.VMEM((ROWS, D), bf),
                   pltpu.VMEM((N * KA, last), bf), pltpu.VMEM((N, KB, COLS), bf)),
        in_specs=[hbm, hbm],
        out_specs=(vmem,) * (NPRE + 3),
        scratch_shapes=[
            *[pltpu.VMEM((N * KA, wid), bf) for wid in WIDS[:NPRE]],
            *[pltpu.VMEM((N * KB, wid), bf) for wid in WIDS[:NPRE]],
            pltpu.VMEM((NP, NZ, BLK, D), bf), pltpu.VMEM((KB, N * COLS), bf),
            pltpu.SemaphoreType.REGULAR((4,)), dma((2,)), dma, dma, dma, dma, dma, dma((NCH,)), dma((NCH,)), dma, dma,
        ],
        compiler_params=pltpu.CompilerParams(
            collective_id=0, has_side_effects=True, vmem_limit_bytes=19 * 2**20),
        name="exchange",
    )(pltpu.with_memory_space_constraint(h, pltpu.HBM), w)
    return pl.pallas_call(
        finish,
        out_shape=jax.ShapeDtypeStruct((ROWS, COLS), bf),
        in_specs=[vmem] * (NPRE + 3),
        out_specs=any_,
        scratch_shapes=[pltpu.VMEM((N * KB, last), bf), pltpu.VMEM((ROWS, last), bf), dma((NPRE, ROWS // TM)), dma((ROWS // TM,))],
        compiler_params=pltpu.CompilerParams(vmem_limit_bytes=19 * 2**20),
        name="finish",
    )(*passed)


def solution(mesh):
    return jax.shard_map(
        local_part,
        mesh=mesh,
        in_specs=(P(("dp", "tp"), None), P(("dp", "tp"), None)),
        out_specs=P(None, ("dp", "tp")),
        check_vma=False,
    )
```

```python
import jax
import jax.numpy as jnp
from jax import lax
from jax.experimental import pallas as pl
from jax.experimental.pallas import tpu as pltpu
from jax.sharding import PartitionSpec as P

MESH = pl.DeviceIdType.MESH
NZ, NP = 4, 8
N = NZ * NP
ROWS, BLK, D = 2048, 64, 640
KA = 16
KB = 4
COLS = 8192
WIDS = (2560, 2560, 2048, 1024)
OFFS = tuple(sum(WIDS[:c]) for c in range(len(WIDS)))
NCH = len(WIDS)
NPRE = NCH - 1
LOOK = 2
AHEAD = 3
TN = 256
TM = 512

MSEQ = (0, 2, 4, 3, 1, 6, 5, 7)
ORDER = [(kz, m) for m in range(NP) for kz in (2, 1, 3, 0) if (kz, m) != (0, 0)]
EARLY = [(0, 2), (0, 4), (0, 3), (0, 1), (1, 0)]


def plane(kz):
    return [(kz, m) for m in MSEQ if (kz, m) != (0, 0)]


def product(hp_ref, ra, rb, m, n):
    a = jnp.dot(hp_ref[m, 0 : N * KA], ra[:, n], preferred_element_type=jnp.float32)
    b = jnp.dot(hp_ref[m, N * KA : D], rb[:, n], preferred_element_type=jnp.float32)
    return (a + b).astype(jnp.bfloat16)


def exchange(h_ref, w_ref, *refs):
    ys, (hp_ref, ra_last, rb_last), refs = refs[:NPRE], refs[NPRE : NPRE + 3], refs[NPRE + 3 :]
    ras, rbs, rbps, refs = refs[:NPRE], refs[NPRE : 2 * NPRE], refs[2 * NPRE : 3 * NPRE], refs[3 * NPRE :]
    hraw, bsrc, news, loc, hz_s, hm_r, hn_r, hp_s, hp_r, a_s, a_r, b_s, b_r = refs
    ras, rbs = (*ras, ra_last), (*rbs, rb_last)
    i, j = lax.axis_index("dp"), lax.axis_index("tp")
    me = i * NP + j
    inner = jnp.logical_and(i >= 1, i <= 2)

    bcopy = pltpu.make_async_copy(w_ref.at[KA : KA + KB, :], bsrc, loc.at[0])
    bcopy.start()
    hown = pltpu.make_async_copy(h_ref, hraw.at[j, i], loc.at[1])
    hown.start()

    barrier = pltpu.get_barrier_semaphore()

    def peer(kz, kp):
        return {"dp": i ^ kz, "tp": j ^ kp}

    def tell(sem, kz, kp=0):
        pl.semaphore_signal(sem, inc=1, device_id=peer(kz, kp), device_id_type=MESH)

    @pl.when(inner)
    def _():
        tell(barrier, 3)
        tell(barrier, 1)
        pl.semaphore_wait(barrier, 1)

    @pl.when(jnp.logical_not(inner))
    def _():
        for kz, kp in plane(0):
            tell(barrier, kz, kp)
        pl.semaphore_wait(barrier, NP)

    def remote(src, dst, s, r, to):
        return pltpu.make_async_remote_copy(src, dst, s, r, device_id=to, device_id_type=MESH)

    def cols(dev, c):
        return pl.ds(pl.multiple_of(dev * COLS + OFFS[c], 256), WIDS[c])

    rows_a = pl.ds(pl.multiple_of(me * KA, KA), KA)

    def send_a(c, kz, kp):
        dev = (i ^ kz) * NP + (j ^ kp)
        remote(w_ref.at[0:KA, cols(dev, c)], ras[c].at[rows_a, :], a_s.at[c], a_r.at[c], peer(kz, kp)).start()

    def send_b(c, kz, kp):
        dev = (i ^ kz) * NP + (j ^ kp)
        remote(bsrc.at[:, cols(dev, c)], rbs[c].at[me], b_s.at[c], b_r.at[c], peer(kz, kp)).start()

    def send_list(c, order):
        for kz, kp in order:
            send_a(c, kz, kp)
            send_b(c, kz, kp)

    def send(c):
        if c < AHEAD:
            @pl.when(inner)
            def _():
                send_list(c, [k for k in ORDER if k != (3, 0)])

            @pl.when(jnp.logical_not(inner))
            def _():
                send_list(c, ORDER)
        else:
            send_list(c, ORDER)

        own(c)

    def own(c):
        pltpu.make_async_copy(w_ref.at[0:KA, cols(me, c)], ras[c].at[rows_a, :], a_r.at[c]).start()
        pltpu.make_async_copy(w_ref.at[KA : KA + KB, cols(me, c)], rbs[c].at[me], b_r.at[c]).start()

    def hidden(kz, r):
        remote(h_ref, hraw.at[j, i], hz_s, r, peer(kz, 0)).start()

    @pl.when(inner)
    def _():
        hidden(3, hm_r)
        for c in range(AHEAD):
            send_a(c, 3, 0)
        bcopy.wait()
        for c in range(AHEAD):
            send_b(c, 3, 0)
        pl.semaphore_wait(news.at[1], 1)
        tell(news.at[2], 3)
        hidden(1, hn_r)
        pl.semaphore_wait(news.at[2], 1)
        tell(news.at[3], 1)
        send_list(0, [k for k in ORDER if k != (3, 0)])

    @pl.when(jnp.logical_not(inner))
    def _():
        for kz, kp in plane(0):
            tell(news.at[0], kz, kp)
        hidden(1, hn_r)
        bcopy.wait()
        send_list(0, EARLY[:4])
        pl.semaphore_wait(news.at[0], NP - 1)
        tell(news.at[1], 1)
        send_list(0, EARLY[4:])
        pl.semaphore_wait(news.at[3], 1)
        hidden(3, hm_r)
        send_list(0, [k for k in ORDER if k not in EARLY])

    own(0)
    got = hraw.at[j, NZ - 1 - i]
    pltpu.make_async_copy(got, got, hm_r).wait()
    remote(got, got, hz_s, hn_r, peer(1, 0)).start()
    hown.wait()
    pltpu.make_async_copy(hraw.at[j, 0:2], hraw.at[j, 0:2], hn_r).wait()
    for kp in range(1, NP):
        remote(hraw.at[j], hraw.at[j], hp_s, hp_r, peer(0, kp)).start()
    for c in range(1, LOOK):
        send(c)

    pltpu.make_async_copy(hraw.at[0 : NP - 1], hraw.at[0 : NP - 1], hp_r).wait()
    row = lax.broadcasted_iota(jnp.int32, (D, D), 0)
    col = lax.broadcasted_iota(jnp.int32, (D, D), 1)
    src = (row * 3277) >> 16
    r = row - src * (KA + KB)
    to = jnp.where(r < KA, src * KA + r, N * KA + src * KB + r - KA)
    perm = jnp.where(to == col, 1.0, 0.0).astype(jnp.bfloat16)
    for p in range(NP):
        x = hraw[p].reshape(NZ * BLK, D)
        x = jnp.dot(x, perm, preferred_element_type=jnp.float32).astype(jnp.bfloat16)
        for z in range(NZ):
            hp_ref[pl.ds((z * NP + p) * BLK, BLK), :] = x[z * BLK : (z + 1) * BLK]

    for c in range(NCH):
        pltpu.make_async_copy(ras[c], ras[c], a_r.at[c]).wait()
        pltpu.make_async_copy(rbs[c], rbs[c], b_r.at[c]).wait()
        if c + LOOK < NCH:
            send(c + LOOK)
        if c < NPRE:
            rbps[c][...] = rbs[c][...].reshape(N * KB, WIDS[c])

            @pl.loop(0, WIDS[c] // TN)
            def _(t):
                n = pl.ds(pl.multiple_of(t * TN, TN), TN)

                @pl.loop(0, ROWS // TM)
                def _(u):
                    m = pl.ds(pl.multiple_of(u * TM, TM), TM)
                    ys[c][m, n] = product(hp_ref, ras[c], rbps[c], m, n)

    pltpu.make_async_copy(hraw.at[0, 0:3], hraw.at[0, 0:3], hz_s).wait()
    pltpu.make_async_copy(hraw.at[0 : NP - 1], hraw.at[0 : NP - 1], hp_s).wait()
    for c in range(NCH):
        part = ras[c].at[0 : (N - 1) * KA, :]
        pltpu.make_async_copy(part, part, a_s.at[c]).wait()
        part = rbs[c].at[0 : N - 1]
        pltpu.make_async_copy(part, part, b_s.at[c]).wait()


def finish(*refs):
    ys, (hp_ref, ra, rb, out_ref, rbp, ybuf, sem_pre, sem) = refs[:NPRE], refs[NPRE:]
    copies = []

    def put(src, u, c, s):
        m = pl.ds(u * TM, TM)
        copy = pltpu.make_async_copy(src.at[m, :], out_ref.at[m, OFFS[c] : OFFS[c] + WIDS[c]], s)
        copy.start(priority=len(copies) % 2)
        copies.append(copy)

    for u in range(ROWS // TM):
        for c, y in enumerate(ys):
            put(y, u, c, sem_pre.at[c, u])
    rbp[...] = rb[...].reshape(N * KB, WIDS[-1])
    for u in range(ROWS // TM):
        m = pl.ds(u * TM, TM)

        @pl.loop(0, WIDS[-1] // TN)
        def _(t):
            n = pl.ds(pl.multiple_of(t * TN, TN), TN)
            ybuf[m, n] = product(hp_ref, ra, rbp, m, n)

        put(ybuf, u, NCH - 1, sem.at[u])
    for copy in copies:
        copy.wait()


def local_part(h, w):
    bf = jnp.bfloat16
    any_, vmem = pl.BlockSpec(memory_space=pl.ANY), pl.BlockSpec(memory_space=pltpu.VMEM)
    hbm = pl.BlockSpec(memory_space=pltpu.HBM)
    dma = pltpu.SemaphoreType.DMA
    last = WIDS[-1]
    passed = pl.pallas_call(
        exchange,
        out_shape=(*[pltpu.VMEM((ROWS, wid), bf) for wid in WIDS[:NPRE]], pltpu.VMEM((ROWS, D), bf),
                   pltpu.VMEM((N * KA, last), bf), pltpu.VMEM((N, KB, last), bf)),
        in_specs=[hbm, hbm],
        out_specs=(vmem,) * (NPRE + 3),
        scratch_shapes=[
            *[pltpu.VMEM((N * KA, wid), bf) for wid in WIDS[:NPRE]],
            *[pltpu.VMEM((N, KB, wid), bf) for wid in WIDS[:NPRE]],
            *[pltpu.VMEM((N * KB, wid), bf) for wid in WIDS[:NPRE]],
            pltpu.VMEM((NP, NZ, BLK, D), bf), pltpu.VMEM((KB, N * COLS), bf),
            pltpu.SemaphoreType.REGULAR((4,)), dma((2,)), dma, dma, dma, dma, dma, dma((NCH,)), dma((NCH,)), dma((NCH,)), dma((NCH,)),
        ],
        compiler_params=pltpu.CompilerParams(
            collective_id=0, has_side_effects=True, vmem_limit_bytes=19 * 2**20),
        name="exchange",
    )(pltpu.with_memory_space_constraint(h, pltpu.HBM), w)
    return pl.pallas_call(
        finish,
        out_shape=jax.ShapeDtypeStruct((ROWS, COLS), bf),
        in_specs=[vmem] * (NPRE + 3),
        out_specs=any_,
        scratch_shapes=[pltpu.VMEM((N * KB, last), bf), pltpu.VMEM((ROWS, last), bf), dma((NPRE, ROWS // TM)), dma((ROWS // TM,))],
        compiler_params=pltpu.CompilerParams(vmem_limit_bytes=19 * 2**20),
        name="finish",
    )(*passed)


def solution(mesh):
    return jax.shard_map(
        local_part,
        mesh=mesh,
        in_specs=(P(("dp", "tp"), None), P(("dp", "tp"), None)),
        out_specs=P(None, ("dp", "tp")),
        check_vma=False,
    )
```

```python
import jax
import jax.numpy as jnp
from jax import lax
from jax.experimental import pallas as pl
from jax.experimental.pallas import tpu as pltpu
from jax.sharding import PartitionSpec as P

MESH = pl.DeviceIdType.MESH
NZ, NP = 4, 8
N = NZ * NP
ROWS, BLK, D = 2048, 64, 640
KA = 16
KB = 4
COLS = 8192
WIDS = (2304, 2304, 2048, 1536)
OFFS = tuple(sum(WIDS[:c]) for c in range(len(WIDS)))
NCH = len(WIDS)
NPRE = NCH - 1
LOOK = 2
AHEAD = 3
TN = 256
TM = 512

MSEQ = (0, 2, 4, 3, 1, 6, 5, 7)
ORDER = [(kz, m) for m in range(NP) for kz in (2, 1, 3, 0) if (kz, m) != (0, 0)]
EARLY = [(0, 2), (0, 4), (0, 3), (0, 1), (1, 0)]


def plane(kz):
    return [(kz, m) for m in MSEQ if (kz, m) != (0, 0)]


def product(hp_ref, ra, rb, m, n):
    a = jnp.dot(hp_ref[m, 0 : N * KA], ra[:, n], preferred_element_type=jnp.float32)
    b = jnp.dot(hp_ref[m, N * KA : D], rb[:, n], preferred_element_type=jnp.float32)
    return (a + b).astype(jnp.bfloat16)


def exchange(h_ref, w_ref, *refs):
    ys, (hp_ref, ra_last, rb_last), refs = refs[:NPRE], refs[NPRE : NPRE + 3], refs[NPRE + 3 :]
    ras, rbs, rbps, refs = refs[:NPRE], refs[NPRE : 2 * NPRE], refs[2 * NPRE : 3 * NPRE], refs[3 * NPRE :]
    hraw, bsrc, news, loc, hz_s, hm_r, hn_r, hp_s, hp_r, a_s, a_r, b_s, b_r = refs
    ras, rbs = (*ras, ra_last), (*rbs, rb_last)
    i, j = lax.axis_index("dp"), lax.axis_index("tp")
    me = i * NP + j
    inner = jnp.logical_and(i >= 1, i <= 2)

    bcopy = pltpu.make_async_copy(w_ref.at[KA : KA + KB, :], bsrc, loc.at[0])
    bcopy.start()
    hown = pltpu.make_async_copy(h_ref, hraw.at[j, i], loc.at[1])
    hown.start()

    barrier = pltpu.get_barrier_semaphore()

    def peer(kz, kp):
        return {"dp": i ^ kz, "tp": j ^ kp}

    def tell(sem, kz, kp=0):
        pl.semaphore_signal(sem, inc=1, device_id=peer(kz, kp), device_id_type=MESH)

    @pl.when(inner)
    def _():
        tell(barrier, 3)
        tell(barrier, 1)
        pl.semaphore_wait(barrier, 1)

    @pl.when(jnp.logical_not(inner))
    def _():
        for kz, kp in plane(0):
            tell(barrier, kz, kp)
        pl.semaphore_wait(barrier, NP)

    def remote(src, dst, s, r, to):
        return pltpu.make_async_remote_copy(src, dst, s, r, device_id=to, device_id_type=MESH)

    def cols(dev, c):
        return pl.ds(pl.multiple_of(dev * COLS + OFFS[c], 256), WIDS[c])

    rows_a = pl.ds(pl.multiple_of(me * KA, KA), KA)

    def send_a(c, kz, kp):
        dev = (i ^ kz) * NP + (j ^ kp)
        remote(w_ref.at[0:KA, cols(dev, c)], ras[c].at[rows_a, :], a_s.at[c], a_r.at[c], peer(kz, kp)).start()

    def send_b(c, kz, kp):
        dev = (i ^ kz) * NP + (j ^ kp)
        remote(bsrc.at[:, cols(dev, c)], rbs[c].at[me], b_s.at[c], b_r.at[c], peer(kz, kp)).start()

    def send_list(c, order):
        for kz, kp in order:
            send_a(c, kz, kp)
            send_b(c, kz, kp)

    def send(c):
        if c < AHEAD:
            @pl.when(inner)
            def _():
                send_list(c, [k for k in ORDER if k != (3, 0)])

            @pl.when(jnp.logical_not(inner))
            def _():
                send_list(c, ORDER)
        else:
            send_list(c, ORDER)

        own(c)

    def own(c):
        pltpu.make_async_copy(w_ref.at[0:KA, cols(me, c)], ras[c].at[rows_a, :], a_r.at[c]).start()
        pltpu.make_async_copy(w_ref.at[KA : KA + KB, cols(me, c)], rbs[c].at[me], b_r.at[c]).start()

    def hidden(kz, r):
        remote(h_ref, hraw.at[j, i], hz_s, r, peer(kz, 0)).start()

    @pl.when(inner)
    def _():
        hidden(3, hm_r)
        for c in range(AHEAD):
            send_a(c, 3, 0)
        bcopy.wait()
        for c in range(AHEAD):
            send_b(c, 3, 0)
        pl.semaphore_wait(news.at[1], 1)
        tell(news.at[2], 3)
        hidden(1, hn_r)
        pl.semaphore_wait(news.at[2], 1)
        tell(news.at[3], 1)
        send_list(0, [k for k in ORDER if k != (3, 0)])

    @pl.when(jnp.logical_not(inner))
    def _():
        for kz, kp in plane(0):
            tell(news.at[0], kz, kp)
        hidden(1, hn_r)
        bcopy.wait()
        send_list(0, EARLY[:4])
        pl.semaphore_wait(news.at[0], NP - 1)
        tell(news.at[1], 1)
        send_list(0, EARLY[4:])
        pl.semaphore_wait(news.at[3], 1)
        hidden(3, hm_r)
        send_list(0, [k for k in ORDER if k not in EARLY])

    own(0)
    got = hraw.at[j, NZ - 1 - i]
    pltpu.make_async_copy(got, got, hm_r).wait()
    remote(got, got, hz_s, hn_r, peer(1, 0)).start()
    hown.wait()
    pltpu.make_async_copy(hraw.at[j, 0:2], hraw.at[j, 0:2], hn_r).wait()
    for kp in range(1, NP):
        remote(hraw.at[j], hraw.at[j], hp_s, hp_r, peer(0, kp)).start()
    for c in range(1, LOOK):
        send(c)

    pltpu.make_async_copy(hraw.at[0 : NP - 1], hraw.at[0 : NP - 1], hp_r).wait()
    row = lax.broadcasted_iota(jnp.int32, (D, D), 0)
    col = lax.broadcasted_iota(jnp.int32, (D, D), 1)
    src = (row * 3277) >> 16
    r = row - src * (KA + KB)
    to = jnp.where(r < KA, src * KA + r, N * KA + src * KB + r - KA)
    perm = jnp.where(to == col, 1.0, 0.0).astype(jnp.bfloat16)
    for p in range(NP):
        x = hraw[p].reshape(NZ * BLK, D)
        x = jnp.dot(x, perm, preferred_element_type=jnp.float32).astype(jnp.bfloat16)
        for z in range(NZ):
            hp_ref[pl.ds((z * NP + p) * BLK, BLK), :] = x[z * BLK : (z + 1) * BLK]

    for c in range(NCH):
        pltpu.make_async_copy(ras[c], ras[c], a_r.at[c]).wait()
        pltpu.make_async_copy(rbs[c], rbs[c], b_r.at[c]).wait()
        if c + LOOK < NCH:
            send(c + LOOK)
        if c < NPRE:
            rbps[c][...] = rbs[c][...].reshape(N * KB, WIDS[c])

            @pl.loop(0, WIDS[c] // TN)
            def _(t):
                n = pl.ds(pl.multiple_of(t * TN, TN), TN)

                @pl.loop(0, ROWS // TM)
                def _(u):
                    m = pl.ds(pl.multiple_of(u * TM, TM), TM)
                    ys[c][m, n] = product(hp_ref, ras[c], rbps[c], m, n)

    pltpu.make_async_copy(hraw.at[0, 0:3], hraw.at[0, 0:3], hz_s).wait()
    pltpu.make_async_copy(hraw.at[0 : NP - 1], hraw.at[0 : NP - 1], hp_s).wait()
    for c in range(NCH):
        part = ras[c].at[0 : (N - 1) * KA, :]
        pltpu.make_async_copy(part, part, a_s.at[c]).wait()
        part = rbs[c].at[0 : N - 1]
        pltpu.make_async_copy(part, part, b_s.at[c]).wait()


def finish(*refs):
    ys, (hp_ref, ra, rb, out_ref, rbp, ybuf, sem_pre, sem) = refs[:NPRE], refs[NPRE:]
    copies = []

    def put(src, u, c, s):
        m = pl.ds(u * TM, TM)
        copy = pltpu.make_async_copy(src.at[m, :], out_ref.at[m, OFFS[c] : OFFS[c] + WIDS[c]], s)
        copy.start(priority=len(copies) % 2)
        copies.append(copy)

    for u in range(ROWS // TM):
        for c, y in enumerate(ys):
            put(y, u, c, sem_pre.at[c, u])
    rbp[...] = rb[...].reshape(N * KB, WIDS[-1])
    for u in range(ROWS // TM):
        m = pl.ds(u * TM, TM)

        @pl.loop(0, WIDS[-1] // TN)
        def _(t):
            n = pl.ds(pl.multiple_of(t * TN, TN), TN)
            ybuf[m, n] = product(hp_ref, ra, rbp, m, n)

        put(ybuf, u, NCH - 1, sem.at[u])
    for copy in copies:
        copy.wait()


def local_part(h, w):
    bf = jnp.bfloat16
    any_, vmem = pl.BlockSpec(memory_space=pl.ANY), pl.BlockSpec(memory_space=pltpu.VMEM)
    hbm = pl.BlockSpec(memory_space=pltpu.HBM)
    dma = pltpu.SemaphoreType.DMA
    last = WIDS[-1]
    passed = pl.pallas_call(
        exchange,
        out_shape=(*[pltpu.VMEM((ROWS, wid), bf) for wid in WIDS[:NPRE]], pltpu.VMEM((ROWS, D), bf),
                   pltpu.VMEM((N * KA, last), bf), pltpu.VMEM((N, KB, last), bf)),
        in_specs=[hbm, hbm],
        out_specs=(vmem,) * (NPRE + 3),
        scratch_shapes=[
            *[pltpu.VMEM((N * KA, wid), bf) for wid in WIDS[:NPRE]],
            *[pltpu.VMEM((N, KB, wid), bf) for wid in WIDS[:NPRE]],
            *[pltpu.VMEM((N * KB, wid), bf) for wid in WIDS[:NPRE]],
            pltpu.VMEM((NP, NZ, BLK, D), bf), pltpu.VMEM((KB, N * COLS), bf),
            pltpu.SemaphoreType.REGULAR((4,)), dma((2,)), dma, dma, dma, dma, dma, dma((NCH,)), dma((NCH,)), dma((NCH,)), dma((NCH,)),
        ],
        compiler_params=pltpu.CompilerParams(
            collective_id=0, has_side_effects=True, vmem_limit_bytes=19 * 2**20),
        name="exchange",
    )(pltpu.with_memory_space_constraint(h, pltpu.HBM), w)
    return pl.pallas_call(
        finish,
        out_shape=jax.ShapeDtypeStruct((ROWS, COLS), bf),
        in_specs=[vmem] * (NPRE + 3),
        out_specs=any_,
        scratch_shapes=[pltpu.VMEM((N * KB, last), bf), pltpu.VMEM((ROWS, last), bf), dma((NPRE, ROWS // TM)), dma((ROWS // TM,))],
        compiler_params=pltpu.CompilerParams(vmem_limit_bytes=19 * 2**20),
        name="finish",
    )(*passed)


def solution(mesh):
    return jax.shard_map(
        local_part,
        mesh=mesh,
        in_specs=(P(("dp", "tp"), None), P(("dp", "tp"), None)),
        out_specs=P(None, ("dp", "tp")),
        check_vma=False,
    )
```
